128 devices in a mesh: seq: 16 (over x, z), head: 8 (over y, core).
Axes of the slice: x: 4, y: 4, z: 4, core: 2. Of those that a mesh axis runs over, the one named last changes fastest.
Arguments:
- queries: bfloat16 [16384, 8192], P('seq', 'head'), may hold values from -0.5390625 to 0.5390625
- keys: bfloat16 [16384, 8192], P('seq', 'head'), may hold values from -0.5390625 to 0.5390625
- values: bfloat16 [16384, 8192], P('seq', 'head'), may hold values from -6 to 6
- log_decay: float32 [16384, 64], P('seq', 'head'), may hold values from -1 to 0
- gain: float32 [8192], P('head'), may hold values from 0.1 to 1.9
- lengths: int32 [8], replicated, may hold values from 1 to 4096, 16384 in all
- out_grad: bfloat16 [16384, 8192], P('seq', 'head'), may hold values from -6 to 6
Outputs:
- normed: bfloat16 [16384, 8192], P('seq', 'head')
- grad_query: bfloat16 [16384, 8192], P('seq', 'head')
- grad_key: bfloat16 [16384, 8192], P('seq', 'head')
- grad_value: bfloat16 [16384, 8192], P('seq', 'head')
The draws below stay inside these ranges and needn't reach their ends.
Inputs may be any that keep to these rules, and one draw needn't show every extreme that they name: The 8 lengths sum to 16384.
All inputs are finite; a program needn't handle non-finite values.
Results may differ from the reference program's by a relative error of at most 0.012.
Values sent between devices are 32-bit elements; how exact they have to be, the bound alone decides.
A program may use at most 128 MiB of HBM per device.

```python
import math
import jax
import jax.numpy as jnp
import numpy as np
from jax import lax

HEAD_COUNT = 64
HD = 128
TOK_DEV = 1024
DOCS = 8
TOKEN_COUNT = 16384


def draw_log_decay(key, part):
    random_subkeys = jax.random.split(jax.random.fold_in(key, 11), 7)
    quick_share = 0.5
    fast_heads = jax.random.uniform(random_subkeys[0], (HEAD_COUNT,)) < quick_share
    slow_rate = jnp.log(10.0) / (3.0 * TOKEN_COUNT) * jax.random.uniform(random_subkeys[1], (HEAD_COUNT,), minval=0.3, maxval=1.0)
    fast_rate = 1.0 / jax.random.uniform(random_subkeys[2], (HEAD_COUNT,), minval=30.0, maxval=50.0)
    decay_rate = jnp.where(fast_heads, fast_rate, slow_rate)
    shards = TOKEN_COUNT // TOK_DEV
    factor = jnp.exp(jax.random.uniform(random_subkeys[3], (shards, 1, HEAD_COUNT), minval=-0.7, maxval=0.7))
    roughness = jax.random.uniform(random_subkeys[4], (shards, TOK_DEV, HEAD_COUNT), minval=0.5, maxval=1.5)
    logarithm_rates = -(decay_rate * factor * roughness).reshape(TOKEN_COUNT, HEAD_COUNT)
    spike_rows = jax.random.randint(random_subkeys[5], (3,), 0, TOKEN_COUNT)
    masked_entries = jnp.any(jnp.arange(TOKEN_COUNT)[:, None] == spike_rows[None, :], axis=1)
    spike_loss = jnp.log(jax.random.uniform(random_subkeys[6], (TOKEN_COUNT, HEAD_COUNT), minval=0.5, maxval=0.8))
    return (logarithm_rates + jnp.where(masked_entries[:, None], spike_loss, 0.0)).astype(jnp.float32)


def steps_of(stream_key, extent, pieces, low, top_value):
    level, own = 1.0, jax.random.fold_in(stream_key, 6)
    for axis_at, shards_of in pieces:
        draws = jnp.exp(jax.random.uniform(jax.random.fold_in(own, axis_at), (shards_of,), jnp.float32, low / len(pieces), top_value / len(pieces)))
        level = level * jnp.repeat(draws, extent[axis_at] // shards_of).reshape([-1 if axis == axis_at else 1 for axis in range(len(extent))])
    return level


def profile(amount, total, reach, slope):
    portions = [(1 << 20) // math.isqrt(grade ** slope) + 1 for grade in range(2, amount + 1)]
    spare, given = total - reach - (amount - 1), [1] * (amount - 1)
    while spare > 0:
        candidates = [i for i in range(amount - 1) if given[i] < reach]
        whole, budget = sum([portions[i] for i in candidates]), spare
        for i in candidates:
            more = min(reach - given[i], max(1, budget * portions[i] // whole), spare)
            given[i] = given[i] + more
            spare = spare - more
    return np.array([reach] + given)


def uneven_parts(stream_key, count, total, most, slope):
    if count == 2:
        one = jax.random.randint(stream_key, (), max(1, total - most), min(most, total - 1) + 1)
        return jnp.stack([one, total - one])
    sizes = jnp.asarray(profile(count, total, most, slope), jnp.int32)
    couples = (count - 1) // 2
    donor, sink = sizes[1:1 + 2 * couples:2], sizes[2:2 + 2 * couples:2]
    slack = jnp.minimum(donor - 1, most - sink)
    moved = jax.random.randint(jax.random.fold_in(stream_key, 1), (couples,), 0, 1 << 20) % (slack + 1)
    sizes = sizes.at[1:1 + 2 * couples:2].set(donor - moved).at[2:2 + 2 * couples:2].set(sink + moved)
    return sizes[jax.random.permutation(jax.random.fold_in(stream_key, 2), count)]


def normal_values(own_key, extent, deviation, limit, cuts=(), kind=jnp.bfloat16):
    entries = deviation * jax.random.normal(own_key, extent, jnp.float32)
    if cuts:
        entries = entries * steps_of(own_key, extent, cuts, -0.22, 0.18)
    return jnp.clip(entries, -limit, limit).astype(kind)


def setup_inputs(seed: int = 0) -> dict:
    splits = jax.random.split(jax.random.key(seed), 8)
    return {
        "queries": normal_values(splits[0], (TOKEN_COUNT, HEAD_COUNT * HD), 0.09, 0.5390625, ((0, 16), (1, 8))),
        "keys": normal_values(splits[1], (TOKEN_COUNT, HEAD_COUNT * HD), 0.09, 0.5390625, ((0, 16), (1, 8))),
        "values": normal_values(splits[2], (TOKEN_COUNT, HEAD_COUNT * HD), 1.0, 6.0, ((0, 16), (1, 8))),
        "log_decay": draw_log_decay(jax.random.fold_in(splits[7], 71), 0),
        "gain": jnp.clip(1.0 + 0.18 * jax.random.normal(splits[4], (HEAD_COUNT * HD,), jnp.float32), 0.1, 1.9),
        "lengths": uneven_parts(splits[5], DOCS, TOKEN_COUNT, TOKEN_COUNT // 4, 2).astype(jnp.int32),
        "out_grad": normal_values(splits[6], (TOKEN_COUNT, HEAD_COUNT * HD), 1.0, 6.0, ((0, 16), (1, 8))),
    }


exact_mode = lax.Precision.HIGHEST
epsilon = 1e-06

def rounded(array):
    return lax.optimization_barrier(array.astype(jnp.bfloat16)).astype(jnp.float32)

def doc_numbers(lengths, first_row, row_count):
    doc_ends = jnp.cumsum(lengths).astype(jnp.int32)
    places = (first_row + jnp.arange(row_count, dtype=jnp.int32)).astype(jnp.int32)
    counted = lax.optimization_barrier(jnp.sum((places[:, None] >= doc_ends[None, :]).astype(jnp.int32), axis=1)).astype(jnp.int32)
    return jnp.where(places >= 0, counted, -1).astype(jnp.int32)

def edge_factors(logarithm_rates, doc_ids, doc_before):
    running = jnp.cumsum(logarithm_rates, axis=0)
    enter_gain = jnp.exp(running) * (doc_ids == doc_before).astype(running.dtype)[:, None]
    leave_gain = jnp.exp(running[-1][None, :] - running) * (doc_ids == doc_ids[-1]).astype(running.dtype)[:, None]
    keep_gain = jnp.exp(running[-1]) * (doc_ids[-1] == doc_before).astype(running.dtype)
    return (running, enter_gain, leave_gain, keep_gain)

def block_factors(logarithm_rates, doc_ids, doc_before):
    running, enter_gain, leave_gain, keep_gain = edge_factors(logarithm_rates, doc_ids, doc_before)
    block_len = doc_ids.shape[0]
    causal = jnp.arange(block_len)[:, None] >= jnp.arange(block_len)[None, :]
    same_doc = (causal & (doc_ids[:, None] == doc_ids[None, :]))[None]
    log_gap = running.T[:, :, None] - running.T[:, None, :]
    weights = jnp.where(same_doc, jnp.exp(jnp.where(same_doc, log_gap, 0.0)), 0.0)
    return (weights, enter_gain, leave_gain, keep_gain)

def reference(queries, keys, values, log_decay, gain, lengths, out_grad):
    full_width = HEAD_COUNT * HD
    block_len = min(128, TOKEN_COUNT)
    blocks = TOKEN_COUNT // block_len

    def by_heads(array):
        return array.reshape(blocks, block_len, HEAD_COUNT, HD)
    doc_ids = doc_numbers(lengths, 0, TOKEN_COUNT).reshape(blocks, block_len)
    starts = jnp.concatenate([jnp.full((1,), -1, jnp.int32), doc_ids[:-1, -1]]).astype(jnp.int32)
    gains = gain.astype(jnp.float32)
    rate_blocks = log_decay.reshape(blocks, block_len, HEAD_COUNT)

    def forward(states, block_item):
        query_blk, key_blk, value_blk, grad_blk, rate_blk, doc_blk, start_doc = block_item
        query_blk = query_blk.astype(jnp.float32)
        key_blk = key_blk.astype(jnp.float32)
        value_blk = value_blk.astype(jnp.float32)
        weights, enter_gain, leave_gain, keep_gain = block_factors(rate_blk, doc_blk, start_doc)
        state_half = rounded(states)
        probs = rounded(jnp.einsum('shd,thd->hst', query_blk, key_blk, precision=exact_mode) * weights)
        raw_out = jnp.einsum('hst,thd->shd', probs, value_blk, precision=exact_mode)
        raw_out = raw_out + enter_gain[:, :, None] * jnp.einsum('shd,hde->she', query_blk, state_half, precision=exact_mode)
        flattened = raw_out.reshape(block_len, full_width)
        inverse = lax.rsqrt(lax.optimization_barrier(jnp.sum(flattened * flattened, axis=1, keepdims=True)) / full_width + epsilon)
        normed = flattened * inverse * gains
        scaled = grad_blk.astype(jnp.float32) * gains
        projected = lax.optimization_barrier(jnp.sum(scaled * flattened, axis=1, keepdims=True))
        grad_flat = inverse * scaled - flattened * inverse ** 3 * projected / full_width
        grad_raw = rounded(grad_flat).reshape(block_len, HEAD_COUNT, HD)
        mixed = rounded(jnp.einsum('shd,thd->hst', grad_raw, value_blk, precision=exact_mode) * weights)
        grad_query = jnp.einsum('hst,thd->shd', mixed, key_blk, precision=exact_mode)
        grad_query = grad_query + enter_gain[:, :, None] * jnp.einsum('hde,she->shd', state_half, grad_raw, precision=exact_mode)
        update = jnp.einsum('thd,the->hde', rounded(key_blk * leave_gain[:, :, None]), value_blk, precision=exact_mode)
        return (keep_gain[:, None, None] * states + update, (normed, grad_raw, grad_query))
    zero_state = jnp.zeros((HEAD_COUNT, HD, HD), jnp.float32)
    inputs = (by_heads(queries), by_heads(keys), by_heads(values), out_grad.reshape(blocks, block_len, full_width), rate_blocks, doc_ids, starts)
    last_state, (normed, grad_raw, grad_query) = lax.scan(forward, zero_state, inputs)

    def backward(carried, block_item):
        query_blk, key_blk, value_blk, rate_blk, doc_blk, start_doc, grad_blk = block_item
        query_blk = query_blk.astype(jnp.float32)
        key_blk = key_blk.astype(jnp.float32)
        value_blk = value_blk.astype(jnp.float32)
        weights, enter_gain, leave_gain, keep_gain = block_factors(rate_blk, doc_blk, start_doc)
        carried_half = rounded(carried)
        probs = rounded(jnp.einsum('shd,thd->hst', query_blk, key_blk, precision=exact_mode) * weights)
        mixed = rounded(jnp.einsum('shd,thd->hst', grad_blk, value_blk, precision=exact_mode) * weights)
        grad_key = jnp.einsum('hst,shd->thd', mixed, query_blk, precision=exact_mode)
        grad_key = grad_key + leave_gain[:, :, None] * jnp.einsum('hde,the->thd', carried_half, value_blk, precision=exact_mode)
        grad_value = jnp.einsum('hst,she->the', probs, grad_blk, precision=exact_mode)
        grad_value = grad_value + leave_gain[:, :, None] * jnp.einsum('hde,thd->the', carried_half, key_blk, precision=exact_mode)
        update = jnp.einsum('shd,she->hde', rounded(query_blk * enter_gain[:, :, None]), grad_blk, precision=exact_mode)
        return (keep_gain[:, None, None] * carried + update, (grad_key, grad_value))
    back_inputs = (by_heads(queries), by_heads(keys), by_heads(values), rate_blocks, doc_ids, starts, grad_raw)
    first_carry, (grad_key, grad_value) = lax.scan(backward, zero_state, back_inputs, reverse=True)
    shape_out = (TOKEN_COUNT, full_width)
    return (normed.reshape(shape_out).astype(jnp.bfloat16), grad_query.reshape(shape_out).astype(jnp.bfloat16), grad_key.reshape(shape_out).astype(jnp.bfloat16), grad_value.reshape(shape_out).astype(jnp.bfloat16))
```

```python
import functools

import jax
import jax.numpy as jnp
from jax import lax
from jax.experimental import pallas as pl
from jax.experimental.pallas import tpu as pltpu
from jax.sharding import Mesh
from jax.sharding import PartitionSpec as P

BLOCK = 128
SEQ = ("x", "z")
MESH = pl.DeviceIdType.MESH
F32 = jnp.float32
BF16 = jnp.bfloat16
epsilon = 1e-06
MASKED = -1e30
SLAB = 2 * BLOCK + 8


def dot(left, right, left_axis=1, right_axis=0):
    dims = (((left_axis,), (right_axis,)), ((), ()))
    return lax.dot_general(left, right, dims, preferred_element_type=F32)


def rows_of(block):
    return pl.ds(pl.multiple_of(block * BLOCK, BLOCK), BLOCK)


def lanes_of(head):
    return slice(head * BLOCK, (head + 1) * BLOCK)


def as_columns(row):
    return jnp.transpose(jnp.broadcast_to(row, (BLOCK, BLOCK)))


def place(linear, head):
    linear = lax.rem(linear + 32, 16)
    return (lax.div(linear, 4), lax.rem(linear, 4), head)


class Exchange:
    def __init__(self, step, own, first_in, totals, near_in, far_in, back, result, send, recv):
        self.own, self.first_in, self.totals, self.near_in = own, first_in, totals, near_in
        self.far_in, self.back, self.result = far_in, back, result
        x, z, head = lax.axis_index("x"), lax.axis_index("z"), lax.axis_index("head")
        me = x * 4 + z
        odd = lax.rem(z, 2)
        outer = jnp.where((z == 0) | (z == 3), 0, 1)
        lower = jnp.where(z < 2, 2, 3)
        self.mine = (outer, lower)
        self.other = (1 - outer, 5 - lower)
        second = (odd == 1, odd == 0)
        self.lead = second if step == 1 else (odd == 0, odd == 1)
        partner = (me + 1 - 2 * odd, me - 1 + 2 * odd)
        near = [me + step * jnp.where(lead, 1, 3) for lead in self.lead]
        far = me + 4 * step

        def copy(source, target, index, linear):
            return pltpu.make_async_remote_copy(
                src_ref=source,
                dst_ref=target,
                send_sem=send.at[index],
                recv_sem=recv.at[index],
                device_id=place(linear, head),
                device_id_type=MESH,
            )

        self.one, self.near, self.far, self.three = [], [], [], []
        for i in range(2):
            self.one.append(copy(own.at[self.other[i]], first_in.at[i], i, partner[i]))
            self.near.append(copy(totals.at[i], near_in.at[i], 2 + i, near[i]))
            self.far.append(copy(totals.at[i], far_in.at[i], 4 + i, far))
            self.three.append(copy(back.at[i], result.at[self.mine[i]], 6 + i, partner[i]))

    def start(self):
        for i in range(2):
            self.one[i].start()

    def sides(self, i):
        mine, theirs, lead = self.own[self.mine[i]], self.first_in[i], self.lead[i]
        return jnp.where(lead, mine, theirs), jnp.where(lead, theirs, mine)

    def scale(self, state, keeps):
        return jnp.concatenate(
            [state[j * BLOCK : (j + 1) * BLOCK] * keeps[2 * BLOCK + j : 2 * BLOCK + j + 1] for j in range(2)]
        )

    def pair_totals(self):
        for i in range(2):
            self.one[i].wait_recv()
            lead, trail = self.sides(i)
            self.totals[i, : 2 * BLOCK] = lead[: 2 * BLOCK] + self.scale(trail, lead)
            self.totals[i, 2 * BLOCK :] = lead[2 * BLOCK :] * trail[2 * BLOCK :]
            self.near[i].start()
            self.far[i].start()

    def edges(self):
        for i in range(2):
            self.near[i].wait_recv()
            self.far[i].wait_recv()
            near = self.near_in[i]
            entering = near[: 2 * BLOCK] + self.scale(self.far_in[i], near)
            _, trail = self.sides(i)
            at_lead = trail[: 2 * BLOCK] + self.scale(entering, trail)
            self.result[self.mine[i]] = jnp.where(self.lead[i], at_lead, entering)
            self.back[i] = jnp.where(self.lead[i], entering, at_lead)
            self.three[i].start()

    def finish(self):
        for i in range(2):
            self.three[i].wait_recv()
        for i in range(2):
            for copies in (self.one, self.near, self.far, self.three):
                copies[i].wait_send()


def state_rows(head):
    return head // 2, slice(head % 2 * BLOCK, (head % 2 + 1) * BLOCK)


def main_kernel(
    full_width,
    lengths, rates, gain, queries, keys, values, out_grad,
    normed, grad_query, key_part, value_part, key_out, value_out, carried_local, beyond, after,
    query, key, value, cotangent, raw, weights, probs, query_in, grad_raw, state_local, state_half,
    running, entering_gain, leaving_gain, keeping, before, documents,
    own_f, first_f, totals_f, near_f, far_f, back_f, entering,
    own_b, first_b, totals_b, near_b, far_b, back_b,
    sums, sums_in, sums_all,
    load_sem, send_f, recv_f, send_b, recv_b, send_h, recv_h,
):
    heads, blocks = 8, 8
    x, z, head = lax.axis_index("x"), lax.axis_index("z"), lax.axis_index("head")
    me = x * 4 + z
    loads = [
        pltpu.make_async_copy(source, target, load_sem.at[i])
        for i, (source, target) in enumerate(
            ((keys, key), (values, value), (queries, query), (out_grad, cotangent))
        )
    ]
    for load in loads:
        load.start()
    barrier = pltpu.get_barrier_semaphore()
    peers = [place(me + step, head) for step in (1, -1, 3, -3, 4, -4)]
    peers += [(x, z, lax.rem(head + j, 8)) for j in range(1, 8)]
    for peer in peers:
        pl.semaphore_signal(barrier, inc=1, device_id=peer, device_id_type=MESH)

    lane = lax.broadcasted_iota(jnp.int32, (BLOCK, BLOCK), 1)
    sublane = lax.broadcasted_iota(jnp.int32, (BLOCK, BLOCK), 0)
    upto = (sublane <= lane).astype(F32).astype(BF16)
    rate = jnp.concatenate([rates[:, lanes_of(b)] for b in range(blocks)])
    top = rate.astype(BF16)
    rest = rate - top.astype(F32)
    middle = rest.astype(BF16)
    low = (rest - middle.astype(F32)).astype(BF16)
    pieces = dot(jnp.concatenate([top, middle, low]), upto)
    count = heads * blocks
    run = pieces[:count] + pieces[count : 2 * count] + pieces[2 * count :]
    block_start = (x * 4 + z) * (blocks * BLOCK) + BLOCK * lax.broadcasted_iota(jnp.int32, (blocks, BLOCK), 0)
    places = block_start + lax.broadcasted_iota(jnp.int32, (blocks, BLOCK), 1)
    doc = jnp.zeros((blocks, BLOCK), jnp.int32)
    doc_first, doc_last = doc, doc
    end = jnp.int32(0)
    for i in range(lengths.shape[0]):
        end = end + lengths[i]
        doc += (places >= end).astype(jnp.int32)
        doc_first += (block_start - 1 >= end).astype(jnp.int32)
        doc_last += (block_start + (BLOCK - 1) >= end).astype(jnp.int32)
    doc_first = jnp.where(block_start > 0, doc_first, -1)
    documents[...] = doc.astype(F32)
    enter_mask = (doc == doc_first).astype(F32)
    leave_mask = (doc == doc_last).astype(F32)
    keep_mask = (doc_last == doc_first).astype(F32)
    so_far = jnp.ones((heads, BLOCK), F32)
    for b in range(blocks):
        run_b = run[b * heads : (b + 1) * heads]
        total = jnp.broadcast_to(run_b[:, BLOCK - 1 :], (heads, BLOCK))
        running[b] = run_b
        entering_gain[b] = jnp.exp(run_b) * enter_mask[b : b + 1]
        leaving_gain[b] = jnp.exp(total - run_b) * leave_mask[b : b + 1]
        keep = jnp.exp(total) * keep_mask[b : b + 1]
        keeping[b] = keep
        before[b] = so_far
        so_far = so_far * keep
    remaining = jnp.ones((heads, BLOCK), F32)
    for b in reversed(range(blocks)):
        after[b] = remaining
        remaining = remaining * keeping[b]
    for s in range(4):
        tile = jnp.concatenate([so_far[2 * s : 2 * s + 2], jnp.zeros((6, BLOCK), F32)])
        own_f[s, 2 * BLOCK :] = tile
        own_b[s, 2 * BLOCK :] = tile

    forward = Exchange(1, own_f, first_f, totals_f, near_f, far_f, back_f, entering, send_f, recv_f)
    backward = Exchange(-1, own_b, first_b, totals_b, near_b, far_b, back_b, beyond, send_b, recv_b)

    loads[0].wait()
    loads[1].wait()
    for h in range(heads):
        state = jnp.zeros((BLOCK, BLOCK), F32)
        for b in range(blocks):
            low_row = b * BLOCK
            key_t = jnp.transpose(key[low_row : low_row + BLOCK, lanes_of(h)]).astype(F32)
            key_t = (key_t * leaving_gain[b, h : h + 1]).astype(BF16)
            state_local[b, h] = state
            state = keeping[b, h : h + 1] * state + dot(key_t, value[low_row : low_row + BLOCK, lanes_of(h)])
        s, part = state_rows(h)
        own_f[s, part] = state
    pl.semaphore_wait(barrier, len(peers))
    forward.start()
    loads[2].wait()
    loads[3].wait()

    def scores(b, carry):
        rows = rows_of(b)
        doc_row = documents[pl.ds(b, 1), :]
        same = (sublane >= lane) & (as_columns(doc_row) == jnp.broadcast_to(doc_row, (BLOCK, BLOCK)))
        bias = jnp.where(same, 0.0, MASKED)
        for h in range(heads):
            lanes = lanes_of(h)
            query_b, key_b = query[rows, lanes], key[rows, lanes]
            run_row = running[b, h : h + 1]
            weight = jnp.exp(as_columns(run_row) - run_row + bias)
            weights[b, h] = weight
            probs[rows, lanes] = (dot(query_b, key_b, 1, 1) * weight).astype(BF16)
            enter = as_columns(entering_gain[b, h : h + 1])
            query_in[rows, lanes] = (query_b.astype(F32) * enter).astype(BF16)
            leave = as_columns(leaving_gain[b, h : h + 1])
            key_out[rows, lanes] = (key_b.astype(F32) * leave).astype(BF16)
            value_out[rows, lanes] = (value[rows, lanes].astype(F32) * leave).astype(BF16)
        return carry

    lax.fori_loop(0, 4, scores, 0)
    forward.pair_totals()
    lax.fori_loop(4, 8, scores, 0)
    forward.edges()
    forward.finish()

    def finish_raw(b, carry):
        rows = rows_of(b)
        squares = jnp.zeros((BLOCK, BLOCK), F32)
        projected = jnp.zeros((BLOCK, BLOCK), F32)
        for h in range(heads):
            lanes = lanes_of(h)
            s, part = state_rows(h)
            state = (state_local[b, h] + before[b, h : h + 1] * entering[s, part]).astype(BF16)
            state_half[b, h] = state
            left = jnp.concatenate([probs[rows, lanes], query_in[rows, lanes]], axis=1)
            right = jnp.concatenate([value[rows, lanes], state])
            out = dot(left, right)
            raw[rows, lanes] = out
            squares += out * out
            projected += out * (cotangent[rows, lanes].astype(F32) * gain[:, lanes])
        sums[0, pl.ds(b, 1)] = jnp.sum(jnp.transpose(squares), axis=0, keepdims=True)
        sums[1, pl.ds(b, 1)] = jnp.sum(jnp.transpose(projected), axis=0, keepdims=True)
        return carry

    lax.fori_loop(0, blocks, finish_raw, 0)
    shares = []
    for j in range(1, 8):
        shares.append(
            pltpu.make_async_remote_copy(
                src_ref=sums,
                dst_ref=sums_in.at[j - 1],
                send_sem=send_h.at[j - 1],
                recv_sem=recv_h.at[j - 1],
                device_id=(x, z, lax.rem(head + j, 8)),
                device_id_type=MESH,
            )
        )
        shares[-1].start()
    total = sums[...]
    for j in range(7):
        shares[j].wait_recv()
        total = total + sums_in[j]
    inverse = lax.rsqrt(total[0] / full_width + epsilon)
    sums_all[0] = inverse
    sums_all[1] = inverse * inverse * inverse * total[1] / full_width
    for j in range(7):
        shares[j].wait_send()

    for h in range(heads):
        s, part = state_rows(h)
        own_b[s, part] = jnp.zeros((BLOCK, BLOCK), F32)

    def norm(step, carry):
        b = blocks - 1 - step
        rows = rows_of(b)
        inverse = as_columns(sums_all[0, pl.ds(b, 1)])
        pull = as_columns(sums_all[1, pl.ds(b, 1)])
        for h in range(heads):
            lanes = lanes_of(h)
            out, gain_h = raw[rows, lanes], gain[:, lanes]
            normed[rows, lanes] = (out * inverse * gain_h).astype(BF16)
            scaled = cotangent[rows, lanes].astype(F32) * gain_h
            grad = (inverse * scaled - out * pull).astype(BF16)
            grad_raw[rows, lanes] = grad
            s, part = state_rows(h)
            carried = own_b[s, part]
            carried_local[b, h] = carried
            own_b[s, part] = keeping[b, h : h + 1] * carried + dot(jnp.transpose(query_in[rows, lanes]), grad)
        return carry

    lax.fori_loop(0, blocks, norm, 0)
    backward.start()

    def gradients(b, carry):
        rows = rows_of(b)
        for h in range(heads):
            lanes = lanes_of(h)
            grad = grad_raw[rows, lanes]
            mixed = (dot(grad, value[rows, lanes], 1, 1) * weights[b, h]).astype(BF16)
            enter = as_columns(entering_gain[b, h : h + 1])
            across = dot(grad, state_half[b, h], 1, 1)
            grad_query[rows, lanes] = (dot(mixed, key[rows, lanes]) + enter * across).astype(BF16)
            key_part[rows, lanes] = dot(jnp.transpose(mixed), query[rows, lanes])
            value_part[rows, lanes] = dot(jnp.transpose(probs[rows, lanes]), grad)
        return carry

    lax.fori_loop(0, 3, gradients, 0)
    backward.pair_totals()
    lax.fori_loop(3, 6, gradients, 0)
    backward.edges()
    lax.fori_loop(6, 8, gradients, 0)
    backward.finish()


def last_kernel(
    normed_in, query_in, key_part, value_part, key_out, value_out, carried_local, beyond, after,
    normed, grad_query, grad_key, grad_value,
    key_rows, value_rows, pass_sem, key_sem, value_sem,
):
    heads, blocks = 8, 8
    passes = [
        pltpu.make_async_copy(normed_in, normed, pass_sem.at[0]),
        pltpu.make_async_copy(query_in, grad_query, pass_sem.at[1]),
    ]
    for copy in passes:
        copy.start()

    def stores(b):
        rows = rows_of(b)
        return (
            pltpu.make_async_copy(key_rows.at[rows], grad_key.at[rows], key_sem.at[b]),
            pltpu.make_async_copy(value_rows.at[rows], grad_value.at[rows], value_sem.at[b]),
        )

    def block(b, carry):
        rows = rows_of(b)
        for h in range(heads):
            lanes = lanes_of(h)
            s, part = state_rows(h)
            carried = (carried_local[b, h] + after[b, h : h + 1] * beyond[s, part]).astype(BF16)
            key_rows[rows, lanes] = (key_part[rows, lanes] + dot(value_out[rows, lanes], carried, 1, 1)).astype(BF16)
            value_rows[rows, lanes] = (value_part[rows, lanes] + dot(key_out[rows, lanes], carried)).astype(BF16)
        for copy in stores(b):
            copy.start()
        return carry

    lax.fori_loop(0, blocks, block, 0)
    for copy in passes:
        copy.wait()

    def settle(b, carry):
        for copy in stores(b):
            copy.wait()
        return carry

    lax.fori_loop(0, blocks, settle, 0)


def body(queries, keys, values, log_decay, gain, lengths, out_grad):
    rows, width = queries.shape
    full_width = width * lax.axis_size("head")
    vmem = pl.BlockSpec(memory_space=pltpu.VMEM)
    hbm = pl.BlockSpec(memory_space=pl.ANY)
    wide = (rows, width)
    tiles = (8, 8, BLOCK, BLOCK)
    small = (8, 8, BLOCK)
    slab = pltpu.VMEM((2, SLAB, BLOCK), F32)
    own = pltpu.VMEM((4, SLAB, BLOCK), F32)
    pair = pltpu.VMEM((2, 2 * BLOCK, BLOCK), F32)
    edge = pltpu.VMEM((4, 2 * BLOCK, BLOCK), F32)
    wires = [own, slab, slab, slab, slab, pair]
    handed = (
        pltpu.VMEM(wide, BF16),
        pltpu.VMEM(wide, BF16),
        pltpu.VMEM(wide, F32),
        pltpu.VMEM(wide, F32),
        pltpu.VMEM(wide, BF16),
        pltpu.VMEM(wide, BF16),
        pltpu.VMEM(tiles, F32),
        edge,
        pltpu.VMEM(small, F32),
    )
    dma = pltpu.SemaphoreType.DMA
    found = pl.pallas_call(
        functools.partial(main_kernel, full_width),
        out_shape=handed,
        in_specs=[pl.BlockSpec(memory_space=pltpu.SMEM), vmem, vmem, hbm, hbm, hbm, hbm],
        out_specs=(vmem,) * len(handed),
        scratch_shapes=[
            pltpu.VMEM(wide, BF16),
            pltpu.VMEM(wide, BF16),
            pltpu.VMEM(wide, BF16),
            pltpu.VMEM(wide, BF16),
            pltpu.VMEM(wide, F32),
            pltpu.VMEM(tiles, F32),
            pltpu.VMEM(wide, BF16),
            pltpu.VMEM(wide, BF16),
            pltpu.VMEM(wide, BF16),
            pltpu.VMEM(tiles, F32),
            pltpu.VMEM(tiles, BF16),
            pltpu.VMEM(small, F32),
            pltpu.VMEM(small, F32),
            pltpu.VMEM(small, F32),
            pltpu.VMEM(small, F32),
            pltpu.VMEM(small, F32),
            pltpu.VMEM((8, BLOCK), F32),
            *wires,
            edge,
            *wires,
            pltpu.VMEM((2, 8, BLOCK), F32),
            pltpu.VMEM((7, 2, 8, BLOCK), F32),
            pltpu.VMEM((2, 8, BLOCK), F32),
            dma((4,)),
            dma((8,)),
            dma((8,)),
            dma((8,)),
            dma((8,)),
            dma((7,)),
            dma((7,)),
        ],
        compiler_params=pltpu.CompilerParams(
            collective_id=0, has_side_effects=True, vmem_limit_bytes=38 * 2**20
        ),
        name="main_kernel",
    )(lengths, log_decay.T, gain.reshape(1, width), queries, keys, values, out_grad)
    return pl.pallas_call(
        last_kernel,
        out_shape=(jax.ShapeDtypeStruct(wide, BF16),) * 4,
        in_specs=[vmem] * len(handed),
        out_specs=(hbm,) * 4,
        scratch_shapes=[
            pltpu.VMEM(wide, BF16),
            pltpu.VMEM(wide, BF16),
            dma((2,)),
            dma((8,)),
            dma((8,)),
        ],
        compiler_params=pltpu.CompilerParams(vmem_limit_bytes=8 * 2**20),
        name="last_kernel",
    )(*found)


def solution(mesh):
    split = Mesh(mesh.devices.reshape(4, 4, mesh.shape["head"]), ("x", "z", "head"))
    wide = P(SEQ, "head")
    return jax.shard_map(
        body,
        mesh=split,
        in_specs=(wide, wide, wide, wide, P("head"), P(), wide),
        out_specs=(wide,) * 4,
        check_vma=False,
    )
```

```python
import functools

import jax
import jax.numpy as jnp
from jax import lax
from jax.experimental import pallas as pl
from jax.experimental.pallas import tpu as pltpu
from jax.sharding import Mesh
from jax.sharding import PartitionSpec as P

BLOCK = 128
HEADS = 8
BLOCKS = 8
SEQ = ("x", "z")
MESH = pl.DeviceIdType.MESH
F32 = jnp.float32
BF16 = jnp.bfloat16
epsilon = 1e-06
MASKED = -1e30
SLAB = BLOCK + 8


def dot(left, right, left_axis=1, right_axis=0):
    dims = (((left_axis,), (right_axis,)), ((), ()))
    return lax.dot_general(left, right, dims, preferred_element_type=F32)


def rows_of(block):
    return pl.ds(pl.multiple_of(block * BLOCK, BLOCK), BLOCK)


def static_rows(block):
    return slice(block * BLOCK, (block + 1) * BLOCK)


def as_columns(row):
    return jnp.transpose(jnp.broadcast_to(row, (BLOCK, BLOCK)))


def place(linear, head):
    linear = lax.rem(linear + 32, 16)
    return (lax.div(linear, 4), lax.rem(linear, 4), head)


class Exchange:
    def __init__(self, step, own, first_in, totals, near_in, far_in, back, result, send, recv):
        self.own, self.first_in, self.totals, self.near_in = own, first_in, totals, near_in
        self.far_in, self.back, self.result = far_in, back, result
        x, z, head = lax.axis_index("x"), lax.axis_index("z"), lax.axis_index("head")
        me = x * 4 + z
        odd = lax.rem(z, 2)
        half = jnp.where((z == 0) | (z == 3), 0, 1)
        self.mine = [4 * half + k for k in range(4)]
        self.other = [4 * (1 - half) + k for k in range(4)]
        self.lead = odd == (1 if step == 1 else 0)
        partner = me + 1 - 2 * odd
        near_to = me + step * jnp.where(self.lead, 1, 3)
        near_from = me - step * jnp.where(self.lead, 3, 1)
        far_to, far_from = me + 4 * step, me - 4 * step

        def exists(linear):
            return (linear >= 0) & (linear < 16)

        self.near_out, self.far_out = exists(near_to), exists(far_to)
        self.near_comes, self.far_comes = exists(near_from), exists(far_from)

        def copy(source, target, index, linear):
            return pltpu.make_async_remote_copy(
                src_ref=source,
                dst_ref=target,
                send_sem=send.at[index],
                recv_sem=recv.at[index],
                device_id=place(linear, head),
                device_id_type=MESH,
            )

        self.one, self.near, self.far, self.three = [], [], [], []
        for k in range(4):
            self.one.append(copy(own.at[self.other[k]], first_in.at[k], k, partner))
            self.near.append(copy(totals.at[k], near_in.at[k], 4 + k, near_to))
            self.far.append(copy(totals.at[k], far_in.at[k], 8 + k, far_to))
            self.three.append(copy(back.at[k], result.at[self.mine[k]], 12 + k, partner))

    def prepare(self):
        @pl.when(jnp.logical_not(self.near_comes))
        def _():
            self.near_in[...] = jnp.zeros_like(self.near_in)

        @pl.when(jnp.logical_not(self.far_comes))
        def _():
            self.far_in[...] = jnp.zeros_like(self.far_in)

    def start(self, k):
        self.one[k].start()

    def sides(self, k):
        mine, theirs = self.own[self.mine[k]], self.first_in[k]
        return jnp.where(self.lead, mine, theirs), jnp.where(self.lead, theirs, mine)

    def pair_totals(self, k):
        self.one[k].wait_recv()
        lead, trail = self.sides(k)
        self.totals[k, :BLOCK] = lead[:BLOCK] + trail[:BLOCK] * lead[BLOCK : BLOCK + 1]
        self.totals[k, BLOCK:] = lead[BLOCK:] * trail[BLOCK:]
        pl.when(self.near_out)(self.near[k].start)
        pl.when(self.far_out)(self.far[k].start)

    def edges(self, k):
        pl.when(self.near_comes)(self.near[k].wait_recv)
        pl.when(self.far_comes)(self.far[k].wait_recv)
        near, far = self.near_in[k], self.far_in[k]
        entering = near[:BLOCK] + far[:BLOCK] * near[BLOCK : BLOCK + 1]
        _, trail = self.sides(k)
        at_lead = trail[:BLOCK] + entering * trail[BLOCK : BLOCK + 1]
        self.back[k] = jnp.where(self.lead, entering, at_lead)
        self.three[k].start()
        self.result[self.mine[k]] = jnp.where(self.lead, at_lead, entering)

    def arrive(self, k):
        self.three[k].wait_recv()

    def finish(self):
        for k in range(4):
            self.one[k].wait_send()
            pl.when(self.near_out)(self.near[k].wait_send)
            pl.when(self.far_out)(self.far[k].wait_send)
            self.three[k].wait_send()


def main_kernel(
    full_width,
    lengths, rates, gain, queries, keys, values, out_grad,
    normed, grad_query, key_part, value_part, key_dev, value_dev, beyond,
    query, key, value, cotangent, raw, scaled, weights, probs_t, query_in_t, query_dev, query_dev_t,
    key_in, grad_raw, state_local, state_half_t, chain, inverse_at, pull_at,
    running, entering_gain, leaving_gain, keeping, before, after, documents,
    own_f, first_f, totals_f, near_f, far_f, back_f, entering,
    own_b, first_b, totals_b, near_b, far_b, back_b,
    sums, sums_in,
    load_sem, send_f, recv_f, send_b, recv_b, send_h, recv_h,
):
    value_in = cotangent
    x, z, head = lax.axis_index("x"), lax.axis_index("z"), lax.axis_index("head")
    me = x * 4 + z
    loads = [
        pltpu.make_async_copy(source, target, load_sem.at[i])
        for i, (source, target) in enumerate(
            ((keys, key), (values, value), (queries, query), (out_grad, cotangent))
        )
    ]
    loads[0].start()
    loads[1].start()
    barrier = pltpu.get_barrier_semaphore()
    peers = [place(me + step, head) for step in (1, -1, 3, -3, 4, -4)]
    peers += [(x, z, lax.rem(head + j, 8)) for j in range(1, 8)]
    for peer in peers:
        pl.semaphore_signal(barrier, inc=1, device_id=peer, device_id_type=MESH)

    lane = lax.broadcasted_iota(jnp.int32, (BLOCK, BLOCK), 1)
    sublane = lax.broadcasted_iota(jnp.int32, (BLOCK, BLOCK), 0)
    upto = (sublane <= lane).astype(F32).astype(BF16)
    rate = jnp.concatenate([rates[:, static_rows(b)] for b in range(BLOCKS)])
    top = rate.astype(BF16)
    rest = rate - top.astype(F32)
    middle = rest.astype(BF16)
    low = (rest - middle.astype(F32)).astype(BF16)
    pieces = dot(jnp.concatenate([top, middle, low]), upto)
    count = HEADS * BLOCKS
    run = pieces[:count] + pieces[count : 2 * count] + pieces[2 * count :]
    block_start = me * (BLOCKS * BLOCK) + BLOCK * lax.broadcasted_iota(jnp.int32, (BLOCKS, BLOCK), 0)
    places = block_start + lax.broadcasted_iota(jnp.int32, (BLOCKS, BLOCK), 1)
    doc = jnp.zeros((BLOCKS, BLOCK), jnp.int32)
    doc_first, doc_last = doc, doc
    end = jnp.int32(0)
    for i in range(lengths.shape[0]):
        end = end + lengths[i]
        doc += (places >= end).astype(jnp.int32)
        doc_first += (block_start - 1 >= end).astype(jnp.int32)
        doc_last += (block_start + (BLOCK - 1) >= end).astype(jnp.int32)
    doc_first = jnp.where(block_start > 0, doc_first, -1)
    documents[...] = doc.astype(F32)
    enter_mask = (doc == doc_first).astype(F32)
    leave_mask = (doc == doc_last).astype(F32)
    keep_mask = (doc_last == doc_first).astype(F32)
    so_far = jnp.ones((HEADS, BLOCK), F32)
    for b in range(BLOCKS):
        run_b = run[b * HEADS : (b + 1) * HEADS]
        total = jnp.broadcast_to(run_b[:, BLOCK - 1 :], (HEADS, BLOCK))
        running[b] = run_b
        entering_gain[b] = jnp.exp(run_b) * enter_mask[b : b + 1]
        leaving_gain[b] = jnp.exp(total - run_b) * leave_mask[b : b + 1]
        keep = jnp.exp(total) * keep_mask[b : b + 1]
        keeping[b] = keep
        before[b] = so_far
        so_far = so_far * keep
    remaining = jnp.ones((HEADS, BLOCK), F32)
    for b in reversed(range(BLOCKS)):
        after[b] = remaining
        remaining = remaining * keeping[b]
    for h in range(HEADS):
        tile = jnp.broadcast_to(so_far[h : h + 1], (8, BLOCK))
        own_f[h, BLOCK:] = tile
        own_b[h, BLOCK:] = tile

    forward = Exchange(1, own_f, first_f, totals_f, near_f, far_f, back_f, entering, send_f, recv_f)
    backward = Exchange(-1, own_b, first_b, totals_b, near_b, far_b, back_b, beyond, send_b, recv_b)

    forward.prepare()
    backward.prepare()

    loads[0].wait()
    loads[1].wait()
    loads[2].start()
    loads[3].start()
    for turn, h in enumerate(forward.other + forward.mine):
        lanes = rows_of(h)
        pieces = []
        for b in range(BLOCKS):
            leave = leaving_gain[b, pl.ds(h, 1)] * after[b, pl.ds(h, 1)]
            pieces.append((jnp.transpose(key[static_rows(b), lanes]).astype(F32) * leave).astype(BF16))
        own_f[h, :BLOCK] = dot(jnp.concatenate(pieces, axis=1), value[:, lanes])
        if turn == 0:
            pl.semaphore_wait(barrier, len(peers))
        if turn < 4:
            forward.start(turn)
    chain[...] = jnp.zeros_like(chain)
    loads[2].wait()
    loads[3].wait()

    def local(b, carry):
        rows = rows_of(b)
        doc_row = documents[pl.ds(b, 1), :]
        same = (sublane >= lane) & (as_columns(doc_row) == jnp.broadcast_to(doc_row, (BLOCK, BLOCK)))
        bias = jnp.where(same, 0.0, MASKED)
        for h in range(HEADS):
            lanes = static_rows(h)
            query_b, key_b, value_b = query[rows, lanes], key[rows, lanes], value[rows, lanes]
            run_row = running[b, h : h + 1]
            weight = jnp.exp(as_columns(run_row) - run_row + bias)
            weights[b, h] = weight
            probs = (dot(query_b, key_b, 1, 1) * weight).astype(BF16)
            probs_t[b, h] = jnp.transpose(probs)
            query_e = query_b.astype(F32) * as_columns(entering_gain[b, h : h + 1])
            query_in = query_e.astype(BF16)
            query_in_t[b, h] = jnp.transpose(query_in)
            query_d = (query_e * before[b, h : h + 1]).astype(BF16)
            query_dev[rows, lanes] = query_d
            query_dev_t[h, :, rows] = jnp.transpose(query_d)
            leave = as_columns(leaving_gain[b, h : h + 1])
            after_row = after[b, h : h + 1]
            key_l = key_b.astype(F32) * leave
            key_lb = key_l.astype(BF16)
            key_in[rows, lanes] = key_lb
            key_dev[rows, lanes] = (key_l * after_row).astype(BF16)
            scaled[rows, lanes] = cotangent[rows, lanes].astype(F32) * gain[:, lanes]
            value_l = value_b.astype(F32) * leave
            value_in[rows, lanes] = value_l.astype(BF16)
            value_dev[rows, lanes] = (value_l * after_row).astype(BF16)
            state = chain[h]
            state_local[b, h] = state
            raw[rows, lanes] = dot(
                jnp.concatenate([probs, query_in], axis=1), jnp.concatenate([value_b, state.astype(BF16)])
            )
            chain[h] = keeping[b, h : h + 1] * state + dot(jnp.transpose(key_lb), value_b)
        return carry

    lax.fori_loop(0, 3, local, 0)
    forward.pair_totals(0)
    forward.pair_totals(1)
    lax.fori_loop(3, 5, local, 0)
    forward.pair_totals(2)
    forward.pair_totals(3)
    lax.fori_loop(5, 8, local, 0)
    squares, projected = inverse_at, pull_at
    squares[...] = jnp.zeros_like(squares)
    projected[...] = jnp.zeros_like(projected)

    def finish_raw(h):
        lanes = rows_of(h)
        added = dot(query_dev[:, lanes], entering[h].astype(BF16))
        for b in range(BLOCKS):
            rows = static_rows(b)
            out = raw[rows, lanes] + added[rows]
            raw[rows, lanes] = out
            squares[b] += out * out
            projected[b] += out * scaled[rows, lanes]

    for k in range(4):
        forward.edges(k)
        finish_raw(forward.mine[k])
    for k in range(4):
        forward.arrive(k)
        finish_raw(forward.other[k])
    for b in range(BLOCKS):
        sums[0, b : b + 1] = jnp.sum(jnp.transpose(squares[b]), axis=0, keepdims=True)
        sums[1, b : b + 1] = jnp.sum(jnp.transpose(projected[b]), axis=0, keepdims=True)
    shares = []
    for j in range(1, 8):
        shares.append(
            pltpu.make_async_remote_copy(
                src_ref=sums,
                dst_ref=sums_in.at[j - 1],
                send_sem=send_h.at[j - 1],
                recv_sem=recv_h.at[j - 1],
                device_id=(x, z, lax.rem(head + j, 8)),
                device_id_type=MESH,
            )
        )
        shares[-1].start()
    forward.finish()
    chain[...] = jnp.zeros_like(chain)

    def whole_states(b, carry):
        for h in range(HEADS):
            state = state_local[b, h] + before[b, h : h + 1] * entering[h]
            state_half_t[b, h] = jnp.transpose(state.astype(BF16))
        return carry

    lax.fori_loop(0, BLOCKS, whole_states, 0)
    total = sums[...]
    for j in range(7):
        shares[j].wait_recv()
        total = total + sums_in[j]
    inverse = lax.rsqrt(total[0] / full_width + epsilon)
    pull = inverse * inverse * inverse * total[1] / full_width
    for b in range(BLOCKS):
        inverse_at[b] = as_columns(inverse[b : b + 1])
        pull_at[b] = as_columns(pull[b : b + 1])
    for turn, h in enumerate(backward.other + backward.mine):
        lanes = rows_of(h)
        pieces = []
        for b in range(BLOCKS):
            rows = static_rows(b)
            grad = (inverse_at[b] * scaled[rows, lanes] - raw[rows, lanes] * pull_at[b]).astype(BF16)
            grad_raw[rows, lanes] = grad
            pieces.append(grad)
        own_b[h, :BLOCK] = dot(query_dev_t[h], jnp.concatenate(pieces))
        if turn < 4:
            backward.start(turn)
    for j in range(7):
        shares[j].wait_send()

    def gradients(step, carry):
        b = BLOCKS - 1 - step
        rows = rows_of(b)
        for h in range(HEADS):
            lanes = static_rows(h)
            grad = grad_raw[rows, lanes]
            mixed = (dot(grad, value[rows, lanes], 1, 1) * weights[b, h]).astype(BF16)
            grad_in = (grad.astype(F32) * as_columns(entering_gain[b, h : h + 1])).astype(BF16)
            grad_query[rows, lanes] = dot(
                jnp.concatenate([mixed, grad_in], axis=1),
                jnp.concatenate([key[rows, lanes], state_half_t[b, h]]),
            ).astype(BF16)
            carried = chain[h]
            carried_half = carried.astype(BF16)
            key_part[rows, lanes] = dot(
                jnp.concatenate([jnp.transpose(mixed), value_in[rows, lanes]], axis=1),
                jnp.concatenate([query[rows, lanes], jnp.transpose(carried_half)]),
            )
            value_part[rows, lanes] = dot(
                jnp.concatenate([probs_t[b, h], key_in[rows, lanes]], axis=1),
                jnp.concatenate([grad, carried_half]),
            )
            chain[h] = keeping[b, h : h + 1] * carried + dot(query_in_t[b, h], grad)
            normed[rows, lanes] = (raw[rows, lanes] * inverse_at[b] * gain[:, lanes]).astype(BF16)
        return carry

    lax.fori_loop(0, 2, gradients, 0)
    backward.pair_totals(0)
    backward.pair_totals(1)
    lax.fori_loop(2, 3, gradients, 0)
    backward.pair_totals(2)
    backward.pair_totals(3)
    lax.fori_loop(3, 6, gradients, 0)
    backward.edges(0)
    lax.fori_loop(6, 7, gradients, 0)
    backward.edges(1)
    lax.fori_loop(7, 8, gradients, 0)
    backward.edges(2)
    backward.edges(3)
    for k in range(4):
        backward.arrive(k)
    backward.finish()


def last_kernel(
    normed_in, query_in, key_part, value_part, key_dev, value_dev, beyond,
    normed, grad_query, grad_key, grad_value,
    key_rows, value_rows, pass_sem, key_sem, value_sem,
):
    passes = [
        pltpu.make_async_copy(normed_in, normed, pass_sem.at[0]),
        pltpu.make_async_copy(query_in, grad_query, pass_sem.at[1]),
    ]
    for copy in passes:
        copy.start()

    def stores(b):
        rows = rows_of(b)
        return (
            pltpu.make_async_copy(key_rows.at[rows], grad_key.at[rows], key_sem.at[b]),
            pltpu.make_async_copy(value_rows.at[rows], grad_value.at[rows], value_sem.at[b]),
        )

    def block(b, carry):
        rows = rows_of(b)
        for h in range(HEADS):
            lanes = static_rows(h)
            carried = beyond[h].astype(BF16)
            key_rows[rows, lanes] = (key_part[rows, lanes] + dot(value_dev[rows, lanes], carried, 1, 1)).astype(BF16)
            value_rows[rows, lanes] = (value_part[rows, lanes] + dot(key_dev[rows, lanes], carried)).astype(BF16)
        for copy in stores(b):
            copy.start()
        return carry

    lax.fori_loop(0, BLOCKS, block, 0)
    for copy in passes:
        copy.wait()

    def settle(b, carry):
        for copy in stores(b):
            copy.wait()
        return carry

    lax.fori_loop(0, BLOCKS, settle, 0)


def body(queries, keys, values, log_decay, gain, lengths, out_grad):
    rows, width = queries.shape
    full_width = width * lax.axis_size("head")
    vmem = pl.BlockSpec(memory_space=pltpu.VMEM)
    hbm = pl.BlockSpec(memory_space=pl.ANY)
    wide = (rows, width)
    tiles = (BLOCKS, HEADS, BLOCK, BLOCK)
    small = pltpu.VMEM((BLOCKS, HEADS, BLOCK), F32)
    own = pltpu.VMEM((HEADS, SLAB, BLOCK), F32)
    slab = pltpu.VMEM((4, SLAB, BLOCK), F32)
    states = pltpu.VMEM((HEADS, BLOCK, BLOCK), F32)
    wires = [own, slab, slab, slab, slab, pltpu.VMEM((4, BLOCK, BLOCK), F32)]
    half, full = pltpu.VMEM(wide, BF16), pltpu.VMEM(wide, F32)
    handed = (half, half, full, full, half, half, states)
    dma = pltpu.SemaphoreType.DMA
    found = pl.pallas_call(
        functools.partial(main_kernel, full_width),
        out_shape=handed,
        in_specs=[pl.BlockSpec(memory_space=pltpu.SMEM), vmem, vmem, hbm, hbm, hbm, hbm],
        out_specs=(vmem,) * len(handed),
        scratch_shapes=[
            half, half, half, half, full, full,
            pltpu.VMEM(tiles, F32),
            pltpu.VMEM(tiles, BF16),
            pltpu.VMEM(tiles, BF16),
            half,
            pltpu.VMEM((HEADS, BLOCK, rows), BF16),
            half, half,
            pltpu.VMEM(tiles, F32),
            pltpu.VMEM(tiles, BF16),
            states, states, states,
            small, small, small, small, small, small,
            pltpu.VMEM((BLOCKS, BLOCK), F32),
            *wires,
            states,
            *wires,
            pltpu.VMEM((2, BLOCKS, BLOCK), F32),
            pltpu.VMEM((7, 2, BLOCKS, BLOCK), F32),
            dma((4,)),
            dma((16,)),
            dma((16,)),
            dma((16,)),
            dma((16,)),
            dma((7,)),
            dma((7,)),
        ],
        compiler_params=pltpu.CompilerParams(
            collective_id=0, has_side_effects=True, vmem_limit_bytes=46 * 2**20
        ),
        name="main_kernel",
    )(lengths, log_decay.T, gain.reshape(1, width), queries, keys, values, out_grad)
    return pl.pallas_call(
        last_kernel,
        out_shape=(jax.ShapeDtypeStruct(wide, BF16),) * 4,
        in_specs=[vmem] * len(handed),
        out_specs=(hbm,) * 4,
        scratch_shapes=[half, half, dma((2,)), dma((8,)), dma((8,))],
        compiler_params=pltpu.CompilerParams(vmem_limit_bytes=8 * 2**20),
        name="last_kernel",
    )(*found)


def solution(mesh):
    split = Mesh(mesh.devices.reshape(4, 4, mesh.shape["head"]), ("x", "z", "head"))
    wide = P(SEQ, "head")
    return jax.shard_map(
        body,
        mesh=split,
        in_specs=(wide, wide, wide, wide, P("head"), P(), wide),
        out_specs=(wide,) * 4,
        check_vma=False,
    )
```

```python
import functools

import jax
import jax.numpy as jnp
from jax import lax
from jax.experimental import pallas as pl
from jax.experimental.pallas import tpu as pltpu
from jax.sharding import Mesh
from jax.sharding import PartitionSpec as P

BLOCK = 128
HEADS = 8
BLOCKS = 8
SEQ = ("x", "z")
MESH = pl.DeviceIdType.MESH
F32 = jnp.float32
BF16 = jnp.bfloat16
epsilon = 1e-06
MASKED = -1e30
SLAB = BLOCK + 8


def dot(left, right, left_axis=1, right_axis=0):
    dims = (((left_axis,), (right_axis,)), ((), ()))
    return lax.dot_general(left, right, dims, preferred_element_type=F32)


def rows_of(block):
    return pl.ds(pl.multiple_of(block * BLOCK, BLOCK), BLOCK)


def static_rows(block):
    return slice(block * BLOCK, (block + 1) * BLOCK)


def as_columns(row):
    return jnp.transpose(jnp.broadcast_to(row, (BLOCK, BLOCK)))


class Exchange:
    def __init__(self, step, own, first_in, totals, mate_in, row, row_in, back, result, send, recv):
        self.own, self.first_in, self.totals, self.mate_in = own, first_in, totals, mate_in
        self.row, self.row_in, self.back, self.result = row, row_in, back, result
        x, z, head = lax.axis_index("x"), lax.axis_index("z"), lax.axis_index("head")
        odd = lax.rem(z, 2)
        half = jnp.where((z == 0) | (z == 3), 0, 1)
        self.mine = [4 * half + k for k in range(4)]
        self.other = [4 * (1 - half) + k for k in range(4)]
        self.lead = odd == (1 if step == 1 else 0)
        self.entry = z < 2 if step == 1 else z >= 2
        self.goes = x < 3 if step == 1 else x > 0
        self.comes = x > 0 if step == 1 else x < 3
        partner = (x, z + 1 - 2 * odd, head)
        mate = (x, 3 - z, head)
        onward = (lax.rem(x + step + 4, 4), z, head)

        def copy(source, target, index, device):
            return pltpu.make_async_remote_copy(
                src_ref=source,
                dst_ref=target,
                send_sem=send.at[index],
                recv_sem=recv.at[index],
                device_id=device,
                device_id_type=MESH,
            )

        self.one, self.two, self.on, self.three = [], [], [], []
        for k in range(4):
            self.one.append(copy(own.at[self.other[k]], first_in.at[k], k, partner))
            self.two.append(copy(totals.at[k], mate_in.at[k], 4 + k, mate))
            self.on.append(copy(row.at[k], row_in.at[k], 8 + k, onward))
            self.three.append(copy(back.at[k], result.at[self.mine[k]], 12 + k, partner))

    def prepare(self):
        @pl.when(jnp.logical_not(self.comes))
        def _():
            self.row_in[...] = jnp.zeros_like(self.row_in)

    def start(self, k):
        self.one[k].start()

    def sides(self, k):
        mine, theirs = self.own[self.mine[k]], self.first_in[k]
        return jnp.where(self.lead, mine, theirs), jnp.where(self.lead, theirs, mine)

    def pair_totals(self, k):
        self.one[k].wait_recv()
        lead, trail = self.sides(k)
        total = lead[:BLOCK] + trail[:BLOCK] * lead[BLOCK : BLOCK + 1]
        self.totals[k, :BLOCK] = total
        self.totals[k, BLOCK:] = lead[BLOCK:] * trail[BLOCK:]
        self.two[k].start()

        @pl.when(jnp.logical_not(self.entry))
        def _():
            self.row[k] = total
            pl.when(self.goes)(self.on[k].start)

    def row_totals(self, k):
        self.two[k].wait_recv()

        @pl.when(self.entry)
        def _():
            mate = self.mate_in[k]
            self.row[k] = mate[:BLOCK] + self.totals[k, :BLOCK] * mate[BLOCK : BLOCK + 1]
            pl.when(self.goes)(self.on[k].start)

    def edges(self, k):
        pl.when(self.comes)(self.on[k].wait_recv)
        mate, row = self.mate_in[k], self.row_in[k]
        entering = jnp.where(self.entry, row, mate[:BLOCK] + row * mate[BLOCK : BLOCK + 1])
        _, trail = self.sides(k)
        at_lead = trail[:BLOCK] + entering * trail[BLOCK : BLOCK + 1]
        self.back[k] = jnp.where(self.lead, entering, at_lead)
        self.three[k].start()
        self.result[self.mine[k]] = jnp.where(self.lead, at_lead, entering)

    def arrive(self, k):
        self.three[k].wait_recv()

    def finish(self):
        for k in range(4):
            self.one[k].wait_send()
            self.two[k].wait_send()
            pl.when(self.goes)(self.on[k].wait_send)
            self.three[k].wait_send()

    def serve(self, step, plan):
        for at, name, k in plan:
            pl.when(step == at)(functools.partial(getattr(self, name), k))


FORWARD_PLAN = (
    (1, "pair_totals", 0),
    (2, "pair_totals", 1),
    (3, "pair_totals", 2),
    (4, "pair_totals", 3),
    (4, "row_totals", 0),
    (5, "row_totals", 1),
    (6, "row_totals", 2),
)
BACKWARD_PLAN = (
    (0, "pair_totals", 0),
    (1, "pair_totals", 1),
    (2, "pair_totals", 2),
    (3, "pair_totals", 3),
    (3, "row_totals", 0),
    (4, "row_totals", 1),
    (4, "row_totals", 2),
    (5, "row_totals", 3),
    (5, "edges", 0),
    (6, "edges", 1),
)


def main_kernel(
    full_width,
    lengths, rates, gain, queries, keys, values, out_grad,
    normed, grad_query, key_part, value_part, key_dev, value_dev, beyond,
    query, key, value, cotangent, raw, scaled, weights, probs_t, query_in_t, query_dev, query_dev_t,
    key_in, grad_raw, state_local, state_half_t, chain, inverse_at, pull_at,
    running, entering_gain, leaving_gain, keeping, before, after, documents,
    own_f, first_f, totals_f, mate_f, row_f, row_in_f, back_f, entering,
    own_b, first_b, totals_b, mate_b, row_b, row_in_b, back_b,
    sums, sums_in,
    load_sem, send_f, recv_f, send_b, recv_b, send_h, recv_h,
):
    value_in = cotangent
    x, z, head = lax.axis_index("x"), lax.axis_index("z"), lax.axis_index("head")
    me = x * 4 + z
    loads = [
        pltpu.make_async_copy(source, target, load_sem.at[i])
        for i, (source, target) in enumerate(
            ((keys, key), (values, value), (queries, query), (out_grad, cotangent))
        )
    ]
    loads[0].start()
    loads[1].start()
    barrier = pltpu.get_barrier_semaphore()
    peers = [(x, z + 1 - 2 * lax.rem(z, 2), head), (x, 3 - z, head)]
    peers += [(lax.rem(x + step, 4), z, head) for step in (1, 3)]
    peers += [(x, z, lax.rem(head + j, 8)) for j in range(1, 8)]
    for peer in peers:
        pl.semaphore_signal(barrier, inc=1, device_id=peer, device_id_type=MESH)

    lane = lax.broadcasted_iota(jnp.int32, (BLOCK, BLOCK), 1)
    sublane = lax.broadcasted_iota(jnp.int32, (BLOCK, BLOCK), 0)
    upto = (sublane <= lane).astype(F32).astype(BF16)
    rate = jnp.concatenate([rates[:, static_rows(b)] for b in range(BLOCKS)])
    top = rate.astype(BF16)
    rest = rate - top.astype(F32)
    middle = rest.astype(BF16)
    low = (rest - middle.astype(F32)).astype(BF16)
    pieces = dot(jnp.concatenate([top, middle, low]), upto)
    count = HEADS * BLOCKS
    run = pieces[:count] + pieces[count : 2 * count] + pieces[2 * count :]
    block_start = me * (BLOCKS * BLOCK) + BLOCK * lax.broadcasted_iota(jnp.int32, (BLOCKS, BLOCK), 0)
    places = block_start + lax.broadcasted_iota(jnp.int32, (BLOCKS, BLOCK), 1)
    doc = jnp.zeros((BLOCKS, BLOCK), jnp.int32)
    doc_first, doc_last = doc, doc
    end = jnp.int32(0)
    for i in range(lengths.shape[0]):
        end = end + lengths[i]
        doc += (places >= end).astype(jnp.int32)
        doc_first += (block_start - 1 >= end).astype(jnp.int32)
        doc_last += (block_start + (BLOCK - 1) >= end).astype(jnp.int32)
    doc_first = jnp.where(block_start > 0, doc_first, -1)
    documents[...] = doc.astype(F32)
    enter_mask = (doc == doc_first).astype(F32)
    leave_mask = (doc == doc_last).astype(F32)
    keep_mask = (doc_last == doc_first).astype(F32)
    so_far = jnp.ones((HEADS, BLOCK), F32)
    for b in range(BLOCKS):
        run_b = run[b * HEADS : (b + 1) * HEADS]
        total = jnp.broadcast_to(run_b[:, BLOCK - 1 :], (HEADS, BLOCK))
        running[b] = run_b
        entering_gain[b] = jnp.exp(run_b) * enter_mask[b : b + 1]
        leaving_gain[b] = jnp.exp(total - run_b) * leave_mask[b : b + 1]
        keep = jnp.exp(total) * keep_mask[b : b + 1]
        keeping[b] = keep
        before[b] = so_far
        so_far = so_far * keep
    remaining = jnp.ones((HEADS, BLOCK), F32)
    for b in reversed(range(BLOCKS)):
        after[b] = remaining
        remaining = remaining * keeping[b]
    for h in range(HEADS):
        tile = jnp.broadcast_to(so_far[h : h + 1], (8, BLOCK))
        own_f[h, BLOCK:] = tile
        own_b[h, BLOCK:] = tile

    forward = Exchange(1, own_f, first_f, totals_f, mate_f, row_f, row_in_f, back_f, entering, send_f, recv_f)
    backward = Exchange(-1, own_b, first_b, totals_b, mate_b, row_b, row_in_b, back_b, beyond, send_b, recv_b)

    forward.prepare()
    backward.prepare()

    loads[0].wait()
    loads[1].wait()
    loads[2].start()
    loads[3].start()
    for turn, h in enumerate(forward.other + forward.mine):
        lanes = rows_of(h)
        pieces = []
        for b in range(BLOCKS):
            leave = leaving_gain[b, pl.ds(h, 1)] * after[b, pl.ds(h, 1)]
            pieces.append((jnp.transpose(key[static_rows(b), lanes]).astype(F32) * leave).astype(BF16))
        own_f[h, :BLOCK] = dot(jnp.concatenate(pieces, axis=1), value[:, lanes])
        if turn == 0:
            pl.semaphore_wait(barrier, len(peers))
        if turn < 4:
            forward.start(turn)
    chain[...] = jnp.zeros_like(chain)
    loads[2].wait()
    loads[3].wait()

    def local(b, carry):
        rows = rows_of(b)
        doc_row = documents[pl.ds(b, 1), :]
        same = (sublane >= lane) & (as_columns(doc_row) == jnp.broadcast_to(doc_row, (BLOCK, BLOCK)))
        bias = jnp.where(same, 0.0, MASKED)
        for h in range(HEADS):
            lanes = static_rows(h)
            query_b, key_b, value_b = query[rows, lanes], key[rows, lanes], value[rows, lanes]
            run_row = running[b, h : h + 1]
            weight = jnp.exp(as_columns(run_row) - run_row + bias)
            weights[b, h] = weight
            probs = (dot(query_b, key_b, 1, 1) * weight).astype(BF16)
            probs_t[b, h] = jnp.transpose(probs)
            query_e = query_b.astype(F32) * as_columns(entering_gain[b, h : h + 1])
            query_in = query_e.astype(BF16)
            query_in_t[b, h] = jnp.transpose(query_in)
            query_d = (query_e * before[b, h : h + 1]).astype(BF16)
            query_dev[rows, lanes] = query_d
            query_dev_t[h, :, rows] = jnp.transpose(query_d)
            leave = as_columns(leaving_gain[b, h : h + 1])
            after_row = after[b, h : h + 1]
            key_l = key_b.astype(F32) * leave
            key_lb = key_l.astype(BF16)
            key_in[rows, lanes] = key_lb
            key_dev[rows, lanes] = (key_l * after_row).astype(BF16)
            scaled[rows, lanes] = cotangent[rows, lanes].astype(F32) * gain[:, lanes]
            value_l = value_b.astype(F32) * leave
            value_in[rows, lanes] = value_l.astype(BF16)
            value_dev[rows, lanes] = (value_l * after_row).astype(BF16)
            state = chain[h]
            state_local[b, h] = state
            raw[rows, lanes] = dot(
                jnp.concatenate([probs, query_in], axis=1), jnp.concatenate([value_b, state.astype(BF16)])
            )
            chain[h] = keeping[b, h : h + 1] * state + dot(jnp.transpose(key_lb), value_b)
        forward.serve(b, FORWARD_PLAN)
        return carry

    lax.fori_loop(0, BLOCKS, local, 0)
    forward.row_totals(3)
    squares, projected = inverse_at, pull_at
    squares[...] = jnp.zeros_like(squares)
    projected[...] = jnp.zeros_like(projected)

    def finish_raw(h):
        lanes = rows_of(h)
        added = dot(query_dev[:, lanes], entering[h].astype(BF16))
        for b in range(BLOCKS):
            rows = static_rows(b)
            out = raw[rows, lanes] + added[rows]
            raw[rows, lanes] = out
            squares[b] += out * out
            projected[b] += out * scaled[rows, lanes]

    for k in range(4):
        forward.edges(k)
        finish_raw(forward.mine[k])
    for k in range(4):
        forward.arrive(k)
        finish_raw(forward.other[k])
    for b in range(BLOCKS):
        sums[0, b : b + 1] = jnp.sum(jnp.transpose(squares[b]), axis=0, keepdims=True)
        sums[1, b : b + 1] = jnp.sum(jnp.transpose(projected[b]), axis=0, keepdims=True)
    shares = []
    for j in range(1, 8):
        shares.append(
            pltpu.make_async_remote_copy(
                src_ref=sums,
                dst_ref=sums_in.at[j - 1],
                send_sem=send_h.at[j - 1],
                recv_sem=recv_h.at[j - 1],
                device_id=(x, z, lax.rem(head + j, 8)),
                device_id_type=MESH,
            )
        )
        shares[-1].start()
    forward.finish()
    chain[...] = jnp.zeros_like(chain)

    def whole_states(b, carry):
        for h in range(HEADS):
            state = state_local[b, h] + before[b, h : h + 1] * entering[h]
            state_half_t[b, h] = jnp.transpose(state.astype(BF16))
        return carry

    lax.fori_loop(0, BLOCKS, whole_states, 0)
    total = sums[...]
    for j in range(7):
        shares[j].wait_recv()
        total = total + sums_in[j]
    inverse = lax.rsqrt(total[0] / full_width + epsilon)
    pull = inverse * inverse * inverse * total[1] / full_width
    for b in range(BLOCKS):
        inverse_at[b] = as_columns(inverse[b : b + 1])
        pull_at[b] = as_columns(pull[b : b + 1])
    for turn, h in enumerate(backward.other + backward.mine):
        lanes = rows_of(h)
        pieces = []
        for b in range(BLOCKS):
            rows = static_rows(b)
            grad = (inverse_at[b] * scaled[rows, lanes] - raw[rows, lanes] * pull_at[b]).astype(BF16)
            grad_raw[rows, lanes] = grad
            pieces.append(grad)
        own_b[h, :BLOCK] = dot(query_dev_t[h], jnp.concatenate(pieces))
        if turn < 4:
            backward.start(turn)
    for j in range(7):
        shares[j].wait_send()

    def gradients(step, carry):
        b = BLOCKS - 1 - step
        rows = rows_of(b)
        for h in range(HEADS):
            lanes = static_rows(h)
            grad = grad_raw[rows, lanes]
            mixed = (dot(grad, value[rows, lanes], 1, 1) * weights[b, h]).astype(BF16)
            grad_in = (grad.astype(F32) * as_columns(entering_gain[b, h : h + 1])).astype(BF16)
            grad_query[rows, lanes] = dot(
                jnp.concatenate([mixed, grad_in], axis=1),
                jnp.concatenate([key[rows, lanes], state_half_t[b, h]]),
            ).astype(BF16)
            carried = chain[h]
            carried_half = carried.astype(BF16)
            key_part[rows, lanes] = dot(
                jnp.concatenate([jnp.transpose(mixed), value_in[rows, lanes]], axis=1),
                jnp.concatenate([query[rows, lanes], jnp.transpose(carried_half)]),
            )
            value_part[rows, lanes] = dot(
                jnp.concatenate([probs_t[b, h], key_in[rows, lanes]], axis=1),
                jnp.concatenate([grad, carried_half]),
            )
            chain[h] = keeping[b, h : h + 1] * carried + dot(query_in_t[b, h], grad)
            normed[rows, lanes] = (raw[rows, lanes] * inverse_at[b] * gain[:, lanes]).astype(BF16)
        backward.serve(step, BACKWARD_PLAN)
        return carry

    lax.fori_loop(0, BLOCKS, gradients, 0)
    backward.edges(2)
    backward.edges(3)
    for k in range(4):
        backward.arrive(k)
    backward.finish()


def last_kernel(
    normed_in, query_in, key_part, value_part, key_dev, value_dev, beyond,
    normed, grad_query, grad_key, grad_value,
    key_rows, value_rows, pass_sem, key_sem, value_sem,
):
    passes = [
        pltpu.make_async_copy(normed_in, normed, pass_sem.at[0]),
        pltpu.make_async_copy(query_in, grad_query, pass_sem.at[1]),
    ]
    for copy in passes:
        copy.start()

    def stores(b):
        rows = rows_of(b)
        return (
            pltpu.make_async_copy(key_rows.at[rows], grad_key.at[rows], key_sem.at[b]),
            pltpu.make_async_copy(value_rows.at[rows], grad_value.at[rows], value_sem.at[b]),
        )

    def block(b, carry):
        rows = rows_of(b)
        for h in range(HEADS):
            lanes = static_rows(h)
            carried = beyond[h].astype(BF16)
            key_rows[rows, lanes] = (key_part[rows, lanes] + dot(value_dev[rows, lanes], carried, 1, 1)).astype(BF16)
            value_rows[rows, lanes] = (value_part[rows, lanes] + dot(key_dev[rows, lanes], carried)).astype(BF16)
        for copy in stores(b):
            copy.start()
        return carry

    lax.fori_loop(0, BLOCKS, block, 0)
    for copy in passes:
        copy.wait()

    def settle(b, carry):
        for copy in stores(b):
            copy.wait()
        return carry

    lax.fori_loop(0, BLOCKS, settle, 0)


def body(queries, keys, values, log_decay, gain, lengths, out_grad):
    rows, width = queries.shape
    full_width = width * lax.axis_size("head")
    vmem = pl.BlockSpec(memory_space=pltpu.VMEM)
    hbm = pl.BlockSpec(memory_space=pl.ANY)
    wide = (rows, width)
    tiles = (BLOCKS, HEADS, BLOCK, BLOCK)
    small = pltpu.VMEM((BLOCKS, HEADS, BLOCK), F32)
    own = pltpu.VMEM((HEADS, SLAB, BLOCK), F32)
    slab = pltpu.VMEM((4, SLAB, BLOCK), F32)
    states = pltpu.VMEM((HEADS, BLOCK, BLOCK), F32)
    part = pltpu.VMEM((4, BLOCK, BLOCK), F32)
    wires = [own, slab, slab, slab, part, part, part]
    half, full = pltpu.VMEM(wide, BF16), pltpu.VMEM(wide, F32)
    handed = (half, half, full, full, half, half, states)
    dma = pltpu.SemaphoreType.DMA
    found = pl.pallas_call(
        functools.partial(main_kernel, full_width),
        out_shape=handed,
        in_specs=[pl.BlockSpec(memory_space=pltpu.SMEM), vmem, vmem, hbm, hbm, hbm, hbm],
        out_specs=(vmem,) * len(handed),
        scratch_shapes=[
            half, half, half, half, full, full,
            pltpu.VMEM(tiles, F32),
            pltpu.VMEM(tiles, BF16),
            pltpu.VMEM(tiles, BF16),
            half,
            pltpu.VMEM((HEADS, BLOCK, rows), BF16),
            half, half,
            pltpu.VMEM(tiles, F32),
            pltpu.VMEM(tiles, BF16),
            states, states, states,
            small, small, small, small, small, small,
            pltpu.VMEM((BLOCKS, BLOCK), F32),
            *wires,
            states,
            *wires,
            pltpu.VMEM((2, BLOCKS, BLOCK), F32),
            pltpu.VMEM((7, 2, BLOCKS, BLOCK), F32),
            dma((4,)),
            dma((16,)),
            dma((16,)),
            dma((16,)),
            dma((16,)),
            dma((7,)),
            dma((7,)),
        ],
        compiler_params=pltpu.CompilerParams(
            collective_id=0, has_side_effects=True, vmem_limit_bytes=46 * 2**20
        ),
        name="main_kernel",
    )(lengths, log_decay.T, gain.reshape(1, width), queries, keys, values, out_grad)
    return pl.pallas_call(
        last_kernel,
        out_shape=(jax.ShapeDtypeStruct(wide, BF16),) * 4,
        in_specs=[vmem] * len(handed),
        out_specs=(hbm,) * 4,
        scratch_shapes=[half, half, dma((2,)), dma((8,)), dma((8,))],
        compiler_params=pltpu.CompilerParams(vmem_limit_bytes=8 * 2**20),
        name="last_kernel",
    )(*found)


def solution(mesh):
    split = Mesh(mesh.devices.reshape(4, 4, mesh.shape["head"]), ("x", "z", "head"))
    wide = P(SEQ, "head")
    return jax.shard_map(
        body,
        mesh=split,
        in_specs=(wide, wide, wide, wide, P("head"), P(), wide),
        out_specs=(wide,) * 4,
        check_vma=False,
    )
```

```python
import functools

import jax
import jax.numpy as jnp
from jax import lax
from jax.experimental import pallas as pl
from jax.experimental.pallas import tpu as pltpu
from jax.sharding import Mesh
from jax.sharding import PartitionSpec as P

BLOCK = 128
HEADS = 8
BLOCKS = 8
SEQ = ("x", "z")
MESH = pl.DeviceIdType.MESH
F32 = jnp.float32
BF16 = jnp.bfloat16
epsilon = 1e-06
MASKED = -1e30
SLAB = BLOCK + 8


def dot(left, right, left_axis=1, right_axis=0):
    dims = (((left_axis,), (right_axis,)), ((), ()))
    return lax.dot_general(left, right, dims, preferred_element_type=F32)


def rows_of(block):
    return pl.ds(pl.multiple_of(block * BLOCK, BLOCK), BLOCK)


def static_rows(block):
    return slice(block * BLOCK, (block + 1) * BLOCK)


def as_columns(row):
    return jnp.transpose(jnp.broadcast_to(row, (BLOCK, BLOCK)))


class Exchange:
    def __init__(self, step, own, first_in, totals, mate_in, row, row_in, back, result, send, recv):
        self.own, self.first_in, self.totals, self.mate_in = own, first_in, totals, mate_in
        self.row, self.row_in, self.back, self.result = row, row_in, back, result
        x, z, head = lax.axis_index("x"), lax.axis_index("z"), lax.axis_index("head")
        odd = lax.rem(z, 2)
        half = jnp.where((z == 0) | (z == 3), 0, 1)
        self.mine = [4 * half + k for k in range(4)]
        self.other = [4 * (1 - half) + k for k in range(4)]
        self.lead = odd == (1 if step == 1 else 0)
        self.entry = z < 2 if step == 1 else z >= 2
        self.goes = x < 3 if step == 1 else x > 0
        self.comes = x > 0 if step == 1 else x < 3
        partner = (x, z + 1 - 2 * odd, head)
        mate = (x, 3 - z, head)
        onward = (lax.rem(x + step + 4, 4), z, head)

        def copy(source, target, index, device):
            return pltpu.make_async_remote_copy(
                src_ref=source,
                dst_ref=target,
                send_sem=send.at[index],
                recv_sem=recv.at[index],
                device_id=device,
                device_id_type=MESH,
            )

        self.one, self.two, self.on, self.three = [], [], [], []
        for k in range(4):
            self.one.append(copy(own.at[self.other[k]], first_in.at[k], k, partner))
            self.two.append(copy(totals.at[k], mate_in.at[k], 4 + k, mate))
            self.on.append(copy(row.at[k], row_in.at[k], 8 + k, onward))
            self.three.append(copy(back.at[k], result.at[self.mine[k]], 12 + k, partner))

    def prepare(self):
        @pl.when(jnp.logical_not(self.comes))
        def _():
            self.row_in[...] = jnp.zeros_like(self.row_in)

    def start(self, k):
        self.one[k].start()

    def sides(self, k):
        mine, theirs = self.own[self.mine[k]], self.first_in[k]
        return jnp.where(self.lead, mine, theirs), jnp.where(self.lead, theirs, mine)

    def pair_totals(self, k):
        self.one[k].wait_recv()
        lead, trail = self.sides(k)
        total = lead[:BLOCK] + trail[:BLOCK] * lead[BLOCK : BLOCK + 1]
        self.totals[k, :BLOCK] = total
        self.totals[k, BLOCK:] = lead[BLOCK:] * trail[BLOCK:]
        self.two[k].start()

        @pl.when(jnp.logical_not(self.entry))
        def _():
            self.row[k] = total
            pl.when(self.goes)(self.on[k].start)

    def row_totals(self, k):
        self.two[k].wait_recv()

        @pl.when(self.entry)
        def _():
            mate = self.mate_in[k]
            self.row[k] = mate[:BLOCK] + self.totals[k, :BLOCK] * mate[BLOCK : BLOCK + 1]
            pl.when(self.goes)(self.on[k].start)

    def edges(self, k):
        pl.when(self.comes)(self.on[k].wait_recv)
        mate, row = self.mate_in[k], self.row_in[k]
        entering = jnp.where(self.entry, row, mate[:BLOCK] + row * mate[BLOCK : BLOCK + 1])
        _, trail = self.sides(k)
        at_lead = trail[:BLOCK] + entering * trail[BLOCK : BLOCK + 1]
        self.back[k] = jnp.where(self.lead, entering, at_lead)
        self.three[k].start()
        self.result[self.mine[k]] = jnp.where(self.lead, at_lead, entering)

    def arrive(self, k):
        self.three[k].wait_recv()

    def finish(self):
        for k in range(4):
            self.one[k].wait_send()
            self.two[k].wait_send()
            pl.when(self.goes)(self.on[k].wait_send)
            self.three[k].wait_send()

    def serve(self, step, plan):
        for at, name, k in plan:
            pl.when(step == at)(functools.partial(getattr(self, name), k))


FORWARD_PLAN = (
    (2, "pair_totals", 0),
    (3, "pair_totals", 1),
    (5, "pair_totals", 2),
    (6, "pair_totals", 3),
    (6, "row_totals", 0),
    (7, "row_totals", 1),
    (9, "row_totals", 2),
    (10, "row_totals", 3),
    (10, "edges", 0),
    (11, "edges", 1),
    (13, "edges", 2),
    (14, "edges", 3),
)
BACKWARD_PLAN = (
    (1, "pair_totals", 0),
    (2, "pair_totals", 1),
    (3, "pair_totals", 2),
    (4, "pair_totals", 3),
    (4, "row_totals", 0),
    (5, "row_totals", 1),
    (6, "row_totals", 2),
    (8, "row_totals", 3),
    (8, "edges", 0),
    (9, "edges", 1),
    (10, "edges", 2),
    (11, "edges", 3),
)


def main_kernel(
    full_width,
    lengths_in, rates_in, gain_in, queries, keys, values, out_grad,
    normed, grad_query, key_part, value_part, key_dev, value_dev, beyond,
    lengths, rates, gain, query, key, value, cotangent, raw, scaled, weights, probs_t, query_in_t, query_dev, query_dev_t,
    key_in, grad_raw, ahead, state_local, state_half_t, chain, inverse_at, pull_at,
    running, entering_gain, leaving_gain, keeping, before, after, documents,
    own_f, first_f, totals_f, mate_f, row_f, row_in_f, back_f, entering,
    own_b, first_b, totals_b, mate_b, row_b, row_in_b, back_b,
    sums, sums_in,
    load_sem, send_f, recv_f, send_b, recv_b, send_h, recv_h,
):
    value_in = cotangent
    x, z, head = lax.axis_index("x"), lax.axis_index("z"), lax.axis_index("head")
    me = x * 4 + z
    half = HEADS // 2 * BLOCK
    mine_first = jnp.where((z == 0) | (z == 3), 0, half)
    first, second = (pl.ds(pl.multiple_of(at, half), half) for at in (half - mine_first, mine_first))
    loads = [
        pltpu.make_async_copy(source, target, load_sem.at[i])
        for i, (source, target) in enumerate(
            (
                (rates_in, rates),
                (lengths_in, lengths),
                (keys.at[:, first], key.at[:, first]),
                (values.at[:, first], value.at[:, first]),
                (keys.at[:, second], key.at[:, second]),
                (values.at[:, second], value.at[:, second]),
                (gain_in, gain),
                (queries, query),
                (out_grad, cotangent),
            )
        )
    ]
    for load in loads[:6]:
        load.start()
    barrier = pltpu.get_barrier_semaphore()
    peers = [(x, z + 1 - 2 * lax.rem(z, 2), head), (x, 3 - z, head)]
    peers += [(lax.rem(x + step, 4), z, head) for step in (1, 3)]
    peers += [(x, z, lax.rem(head + j, 8)) for j in range(1, 8)]
    for peer in peers:
        pl.semaphore_signal(barrier, inc=1, device_id=peer, device_id_type=MESH)

    loads[0].wait()
    loads[1].wait()
    lane = lax.broadcasted_iota(jnp.int32, (BLOCK, BLOCK), 1)
    sublane = lax.broadcasted_iota(jnp.int32, (BLOCK, BLOCK), 0)
    upto = (sublane <= lane).astype(F32).astype(BF16)
    rate = jnp.concatenate([rates[:, static_rows(b)] for b in range(BLOCKS)])
    top = rate.astype(BF16)
    rest = rate - top.astype(F32)
    middle = rest.astype(BF16)
    low = (rest - middle.astype(F32)).astype(BF16)
    pieces = dot(jnp.concatenate([top, middle, low]), upto)
    count = HEADS * BLOCKS
    run = pieces[:count] + pieces[count : 2 * count] + pieces[2 * count :]
    block_start = me * (BLOCKS * BLOCK) + BLOCK * lax.broadcasted_iota(jnp.int32, (BLOCKS, BLOCK), 0)
    places = block_start + lax.broadcasted_iota(jnp.int32, (BLOCKS, BLOCK), 1)
    doc = jnp.zeros((BLOCKS, BLOCK), jnp.int32)
    doc_first, doc_last = doc, doc
    end = jnp.int32(0)
    for i in range(lengths.shape[0]):
        end = end + lengths[i]
        doc += (places >= end).astype(jnp.int32)
        doc_first += (block_start - 1 >= end).astype(jnp.int32)
        doc_last += (block_start + (BLOCK - 1) >= end).astype(jnp.int32)
    doc_first = jnp.where(block_start > 0, doc_first, -1)
    documents[...] = doc.astype(F32)
    enter_mask = (doc == doc_first).astype(F32)
    leave_mask = (doc == doc_last).astype(F32)
    keep_mask = (doc_last == doc_first).astype(F32)
    so_far = jnp.ones((HEADS, BLOCK), F32)
    for b in range(BLOCKS):
        run_b = run[b * HEADS : (b + 1) * HEADS]
        total = jnp.broadcast_to(run_b[:, BLOCK - 1 :], (HEADS, BLOCK))
        running[b] = run_b
        entering_gain[b] = jnp.exp(run_b) * enter_mask[b : b + 1]
        leaving_gain[b] = jnp.exp(total - run_b) * leave_mask[b : b + 1]
        keep = jnp.exp(total) * keep_mask[b : b + 1]
        keeping[b] = keep
        before[b] = so_far
        so_far = so_far * keep
    remaining = jnp.ones((HEADS, BLOCK), F32)
    for b in reversed(range(BLOCKS)):
        after[b] = remaining
        remaining = remaining * keeping[b]
    for h in range(HEADS):
        tile = jnp.broadcast_to(so_far[h : h + 1], (8, BLOCK))
        own_f[h, BLOCK:] = tile
        own_b[h, BLOCK:] = tile

    forward = Exchange(1, own_f, first_f, totals_f, mate_f, row_f, row_in_f, back_f, entering, send_f, recv_f)
    backward = Exchange(-1, own_b, first_b, totals_b, mate_b, row_b, row_in_b, back_b, beyond, send_b, recv_b)

    forward.prepare()
    backward.prepare()

    loads[2].wait()
    loads[3].wait()
    for turn, h in enumerate(forward.other + forward.mine):
        if turn == 4:
            for load in loads[4:6]:
                load.wait()
            for load in loads[6:]:
                load.start()
        lanes = rows_of(h)
        pieces = []
        for b in range(BLOCKS):
            leave = leaving_gain[b, pl.ds(h, 1)] * after[b, pl.ds(h, 1)]
            pieces.append((jnp.transpose(key[static_rows(b), lanes]).astype(F32) * leave).astype(BF16))
        own_f[h, :BLOCK] = dot(jnp.concatenate(pieces, axis=1), value[:, lanes])
        if turn == 0:
            pl.semaphore_wait(barrier, len(peers))
        if turn < 4:
            forward.start(turn)
    chain[...] = jnp.zeros_like(chain)
    for load in loads[6:]:
        load.wait()

    last_step = 2 * BLOCKS - 1

    def local_scores(step):
        b, group = lax.div(step, 2), lax.rem(step, 2)
        rows = rows_of(b)
        doc_row = documents[pl.ds(b, 1), :]
        same = (sublane >= lane) & (as_columns(doc_row) == jnp.broadcast_to(doc_row, (BLOCK, BLOCK)))
        bias = jnp.where(same, 0.0, MASKED)
        for j in range(HEADS // 2):
            h = group * (HEADS // 2) + j
            lanes = rows_of(h)
            query_b, key_b, value_b = query[rows, lanes], key[rows, lanes], value[rows, lanes]
            run_row = running[b, pl.ds(h, 1)]
            weight = jnp.exp(as_columns(run_row) - run_row + bias)
            weights[b, h] = weight
            probs = (dot(query_b, key_b, 1, 1) * weight).astype(BF16)
            ahead[0, j] = probs
            probs_t[b, h] = jnp.transpose(probs)
            query_e = query_b.astype(F32) * as_columns(entering_gain[b, pl.ds(h, 1)])
            query_in = query_e.astype(BF16)
            ahead[1, j] = query_in
            query_in_t[b, h] = jnp.transpose(query_in)
            query_d = (query_e * before[b, pl.ds(h, 1)]).astype(BF16)
            query_dev[rows, lanes] = query_d
            query_dev_t[h, :, rows] = jnp.transpose(query_d)
            leave = as_columns(leaving_gain[b, pl.ds(h, 1)])
            after_row = after[b, pl.ds(h, 1)]
            key_l = key_b.astype(F32) * leave
            key_lb = key_l.astype(BF16)
            key_in[rows, lanes] = key_lb
            ahead[2, j] = jnp.transpose(key_lb)
            key_dev[rows, lanes] = (key_l * after_row).astype(BF16)
            scaled[rows, lanes] = cotangent[rows, lanes].astype(F32) * gain[:, lanes]
            value_l = value_b.astype(F32) * leave
            value_in[rows, lanes] = value_l.astype(BF16)
            value_dev[rows, lanes] = (value_l * after_row).astype(BF16)

    def local(step):
        b, group = lax.div(step, 2), lax.rem(step, 2)
        rows = rows_of(b)
        for j in range(HEADS // 2):
            h = group * (HEADS // 2) + j
            lanes = rows_of(h)
            value_b = value[rows, lanes]
            state = chain[h]
            state_local[b, h] = state
            raw[rows, lanes] = dot(
                jnp.concatenate([ahead[0, j], ahead[1, j]], axis=1), jnp.concatenate([value_b, state.astype(BF16)])
            )
            chain[h] = keeping[b, pl.ds(h, 1)] * state + dot(ahead[2, j], value_b)

    def local_step(step, carry):
        local(step)
        local_scores(step + 1)
        forward.serve(step, FORWARD_PLAN)
        return carry

    local_scores(jnp.int32(0))
    lax.fori_loop(0, last_step, local_step, 0)
    local(jnp.int32(last_step))
    squares, projected = inverse_at, pull_at
    squares[...] = jnp.zeros_like(squares)
    projected[...] = jnp.zeros_like(projected)

    def finish_raw(h):
        lanes = rows_of(h)
        added = dot(query_dev[:, lanes], entering[h].astype(BF16))
        for b in range(BLOCKS):
            rows = static_rows(b)
            out = raw[rows, lanes] + added[rows]
            raw[rows, lanes] = out
            squares[b] += out * out
            projected[b] += out * scaled[rows, lanes]

    for k in range(4):
        finish_raw(forward.mine[k])
    for k in range(4):
        forward.arrive(k)
        finish_raw(forward.other[k])
    for b in range(BLOCKS):
        sums[0, b : b + 1] = jnp.sum(jnp.transpose(squares[b]), axis=0, keepdims=True)
        sums[1, b : b + 1] = jnp.sum(jnp.transpose(projected[b]), axis=0, keepdims=True)
    shares = []
    for j in range(1, 8):
        shares.append(
            pltpu.make_async_remote_copy(
                src_ref=sums,
                dst_ref=sums_in.at[j - 1],
                send_sem=send_h.at[j - 1],
                recv_sem=recv_h.at[j - 1],
                device_id=(x, z, lax.rem(head + j, 8)),
                device_id_type=MESH,
            )
        )
        shares[-1].start()
    forward.finish()
    chain[...] = jnp.zeros_like(chain)

    def whole_states(b, carry):
        for h in range(HEADS):
            state = state_local[b, h] + before[b, h : h + 1] * entering[h]
            state_half_t[b, h] = jnp.transpose(state.astype(BF16))
        return carry

    lax.fori_loop(0, BLOCKS, whole_states, 0)
    total = sums[...]
    for j in range(7):
        shares[j].wait_recv()
        total = total + sums_in[j]
    inverse = lax.rsqrt(total[0] / full_width + epsilon)
    pull = inverse * inverse * inverse * total[1] / full_width
    for b in range(BLOCKS):
        inverse_at[b] = as_columns(inverse[b : b + 1])
        pull_at[b] = as_columns(pull[b : b + 1])
    for turn, h in enumerate(backward.other + backward.mine):
        lanes = rows_of(h)
        pieces = []
        for b in range(BLOCKS):
            rows = static_rows(b)
            grad = (inverse_at[b] * scaled[rows, lanes] - raw[rows, lanes] * pull_at[b]).astype(BF16)
            grad_raw[rows, lanes] = grad
            pieces.append(grad)
        own_b[h, :BLOCK] = dot(query_dev_t[h], jnp.concatenate(pieces))
        if turn < 4:
            backward.start(turn)
    for j in range(7):
        shares[j].wait_send()

    def gradient_scores(step):
        b, group = BLOCKS - 1 - lax.div(step, 2), lax.rem(step, 2)
        rows = rows_of(b)
        for j in range(HEADS // 2):
            h = group * (HEADS // 2) + j
            lanes = rows_of(h)
            grad = grad_raw[rows, lanes]
            mixed = (dot(grad, value[rows, lanes], 1, 1) * weights[b, h]).astype(BF16)
            ahead[0, j] = mixed
            ahead[1, j] = jnp.transpose(mixed)
            ahead[2, j] = (grad.astype(F32) * as_columns(entering_gain[b, pl.ds(h, 1)])).astype(BF16)

    def gradients(step):
        b, group = BLOCKS - 1 - lax.div(step, 2), lax.rem(step, 2)
        rows = rows_of(b)
        for j in range(HEADS // 2):
            h = group * (HEADS // 2) + j
            lanes = rows_of(h)
            grad = grad_raw[rows, lanes]
            grad_query[rows, lanes] = dot(
                jnp.concatenate([ahead[0, j], ahead[2, j]], axis=1),
                jnp.concatenate([key[rows, lanes], state_half_t[b, h]]),
            ).astype(BF16)
            carried = chain[h]
            carried_half = carried.astype(BF16)
            key_part[rows, lanes] = dot(
                jnp.concatenate([ahead[1, j], value_in[rows, lanes]], axis=1),
                jnp.concatenate([query[rows, lanes], jnp.transpose(carried_half)]),
            )
            value_part[rows, lanes] = dot(
                jnp.concatenate([probs_t[b, h], key_in[rows, lanes]], axis=1),
                jnp.concatenate([grad, carried_half]),
            )
            chain[h] = keeping[b, pl.ds(h, 1)] * carried + dot(query_in_t[b, h], grad)
            normed[rows, lanes] = (raw[rows, lanes] * inverse_at[b] * gain[:, lanes]).astype(BF16)

    def gradient_step(step, carry):
        gradients(step)
        gradient_scores(step + 1)
        backward.serve(step, BACKWARD_PLAN)
        return carry

    gradient_scores(jnp.int32(0))
    lax.fori_loop(0, last_step, gradient_step, 0)
    gradients(jnp.int32(last_step))
    for k in range(4):
        backward.arrive(k)
    backward.finish()


def last_kernel(
    normed_in, query_in, key_part, value_part, key_dev, value_dev, beyond,
    normed, grad_query, grad_key, grad_value,
    key_rows, value_rows, plain, turned, pass_sem, key_sem, value_sem,
):
    passes = [
        pltpu.make_async_copy(normed_in, normed, pass_sem.at[0]),
        pltpu.make_async_copy(query_in, grad_query, pass_sem.at[1]),
    ]
    for copy in passes:
        copy.start()

    tall = 2 * BLOCK

    def stores(b):
        rows = pl.ds(pl.multiple_of(b * tall, tall), tall)
        return (
            pltpu.make_async_copy(key_rows.at[rows], grad_key.at[rows], key_sem.at[b]),
            pltpu.make_async_copy(value_rows.at[rows], grad_value.at[rows], value_sem.at[b]),
        )

    zero = jnp.zeros((BLOCK, BLOCK), BF16)
    for h in range(HEADS):
        state = beyond[h].astype(BF16)
        for states, part in ((plain, state), (turned, jnp.transpose(state))):
            pair = (part, zero) if h % 2 == 0 else (zero, part)
            states[h // 2, static_rows(h % 2)] = jnp.concatenate(pair, axis=1)

    def block(b, carry):
        rows = pl.ds(pl.multiple_of(b * tall, tall), tall)
        for pair in range(HEADS // 2):
            lanes = slice(pair * tall, (pair + 1) * tall)
            key_rows[rows, lanes] = (key_part[rows, lanes] + dot(value_dev[rows, lanes], turned[pair])).astype(BF16)
            value_rows[rows, lanes] = (value_part[rows, lanes] + dot(key_dev[rows, lanes], plain[pair])).astype(BF16)
        for copy in stores(b):
            copy.start()
        return carry

    lax.fori_loop(0, BLOCKS // 2, block, 0)
    for copy in passes:
        copy.wait()

    def settle(b, carry):
        for copy in stores(b):
            copy.wait()
        return carry

    lax.fori_loop(0, BLOCKS // 2, settle, 0)


def body(queries, keys, values, log_decay, gain, lengths, out_grad):
    rows, width = queries.shape
    full_width = width * lax.axis_size("head")
    vmem = pl.BlockSpec(memory_space=pltpu.VMEM)
    hbm = pl.BlockSpec(memory_space=pl.ANY)
    wide = (rows, width)
    tiles = (BLOCKS, HEADS, BLOCK, BLOCK)
    small = pltpu.VMEM((BLOCKS, HEADS, BLOCK), F32)
    own = pltpu.VMEM((HEADS, SLAB, BLOCK), F32)
    slab = pltpu.VMEM((4, SLAB, BLOCK), F32)
    states = pltpu.VMEM((HEADS, BLOCK, BLOCK), F32)
    part = pltpu.VMEM((4, BLOCK, BLOCK), F32)
    wires = [own, slab, slab, slab, part, part, part]
    half, full = pltpu.VMEM(wide, BF16), pltpu.VMEM(wide, F32)
    handed = (half, half, full, full, half, half, states)
    two_heads = pltpu.VMEM((HEADS // 2, 2 * BLOCK, 2 * BLOCK), BF16)
    dma = pltpu.SemaphoreType.DMA
    found = pl.pallas_call(
        functools.partial(main_kernel, full_width),
        out_shape=handed,
        in_specs=[hbm] * 7,
        out_specs=(vmem,) * len(handed),
        scratch_shapes=[
            pltpu.SMEM((8,), jnp.int32),
            pltpu.VMEM((HEADS, rows), F32),
            pltpu.VMEM((1, width), F32),
            half, half, half, half, full, full,
            pltpu.VMEM(tiles, F32),
            pltpu.VMEM(tiles, BF16),
            pltpu.VMEM(tiles, BF16),
            half,
            pltpu.VMEM((HEADS, BLOCK, rows), BF16),
            half, half,
            pltpu.VMEM((3, HEADS // 2, BLOCK, BLOCK), BF16),
            pltpu.VMEM(tiles, F32),
            pltpu.VMEM(tiles, BF16),
            states, states, states,
            small, small, small, small, small, small,
            pltpu.VMEM((BLOCKS, BLOCK), F32),
            *wires,
            states,
            *wires,
            pltpu.VMEM((2, BLOCKS, BLOCK), F32),
            pltpu.VMEM((7, 2, BLOCKS, BLOCK), F32),
            dma((9,)),
            dma((16,)),
            dma((16,)),
            dma((16,)),
            dma((16,)),
            dma((7,)),
            dma((7,)),
        ],
        compiler_params=pltpu.CompilerParams(
            collective_id=0, has_side_effects=True, vmem_limit_bytes=46 * 2**20
        ),
        name="main_kernel",
    )(lengths, log_decay.T, gain.reshape(1, width), queries, keys, values, out_grad)
    return pl.pallas_call(
        last_kernel,
        out_shape=(jax.ShapeDtypeStruct(wide, BF16),) * 4,
        in_specs=[vmem] * len(handed),
        out_specs=(hbm,) * 4,
        scratch_shapes=[half, half, two_heads, two_heads, dma((2,)), dma((4,)), dma((4,))],
        compiler_params=pltpu.CompilerParams(vmem_limit_bytes=8 * 2**20),
        name="last_kernel",
    )(*found)


def solution(mesh):
    split = Mesh(mesh.devices.reshape(4, 4, mesh.shape["head"]), ("x", "z", "head"))
    wide = P(SEQ, "head")
    return jax.shard_map(
        body,
        mesh=split,
        in_specs=(wide, wide, wide, wide, P("head"), P(), wide),
        out_specs=(wide,) * 4,
        check_vma=False,
    )
```

```python
import functools

import jax
import jax.numpy as jnp
from jax import lax
from jax.experimental import pallas as pl
from jax.experimental.pallas import tpu as pltpu
from jax.sharding import Mesh
from jax.sharding import PartitionSpec as P

BLOCK = 128
HEADS = 8
BLOCKS = 8
SEQ = ("x", "z")
MESH = pl.DeviceIdType.MESH
F32 = jnp.float32
BF16 = jnp.bfloat16
epsilon = 1e-06
MASKED = -1e30
SLAB = BLOCK + 8


def dot(left, right, left_axis=1, right_axis=0):
    dims = (((left_axis,), (right_axis,)), ((), ()))
    return lax.dot_general(left, right, dims, preferred_element_type=F32)


def rows_of(block):
    return pl.ds(pl.multiple_of(block * BLOCK, BLOCK), BLOCK)


def static_rows(block):
    return slice(block * BLOCK, (block + 1) * BLOCK)


def as_columns(row):
    return jnp.transpose(jnp.broadcast_to(row, (BLOCK, BLOCK)))


class Exchange:
    def __init__(self, step, own, first_in, totals, mate_in, row, row_in, back, result, send, recv):
        self.own, self.first_in, self.totals, self.mate_in = own, first_in, totals, mate_in
        self.row, self.row_in, self.back, self.result = row, row_in, back, result
        x, z, head = lax.axis_index("x"), lax.axis_index("z"), lax.axis_index("head")
        odd = lax.rem(z, 2)
        half = jnp.where((z == 0) | (z == 3), 0, 1)
        self.mine = [4 * half + k for k in range(4)]
        self.other = [4 * (1 - half) + k for k in range(4)]
        self.lead = odd == (1 if step == 1 else 0)
        self.entry = z < 2 if step == 1 else z >= 2
        self.goes = x < 3 if step == 1 else x > 0
        self.comes = x > 0 if step == 1 else x < 3
        partner = (x, z + 1 - 2 * odd, head)
        mate = (x, 3 - z, head)
        onward = (lax.rem(x + step + 4, 4), z, head)

        def copy(source, target, index, device):
            return pltpu.make_async_remote_copy(
                src_ref=source,
                dst_ref=target,
                send_sem=send.at[index],
                recv_sem=recv.at[index],
                device_id=device,
                device_id_type=MESH,
            )

        self.one, self.two, self.on, self.three = [], [], [], []
        for k in range(4):
            self.one.append(copy(own.at[self.other[k]], first_in.at[k], k, partner))
            self.two.append(copy(totals.at[k], mate_in.at[k], 4 + k, mate))
            self.on.append(copy(row.at[k], row_in.at[k], 8 + k, onward))
            self.three.append(copy(back.at[k], result.at[self.mine[k]], 12 + k, partner))

    def prepare(self):
        @pl.when(jnp.logical_not(self.comes))
        def _():
            self.row_in[...] = jnp.zeros_like(self.row_in)

    def start(self, k):
        self.one[k].start()

    def sides(self, k):
        mine, theirs = self.own[self.mine[k]], self.first_in[k]
        return jnp.where(self.lead, mine, theirs), jnp.where(self.lead, theirs, mine)

    def pair_totals(self, k):
        self.one[k].wait_recv()
        lead, trail = self.sides(k)
        total = lead[:BLOCK] + trail[:BLOCK] * lead[BLOCK : BLOCK + 1]
        self.totals[k, :BLOCK] = total
        self.totals[k, BLOCK:] = lead[BLOCK:] * trail[BLOCK:]
        self.two[k].start()

        @pl.when(jnp.logical_not(self.entry))
        def _():
            self.row[k] = total
            pl.when(self.goes)(self.on[k].start)

    def row_totals(self, k):
        self.two[k].wait_recv()

        @pl.when(self.entry)
        def _():
            mate = self.mate_in[k]
            self.row[k] = mate[:BLOCK] + self.totals[k, :BLOCK] * mate[BLOCK : BLOCK + 1]
            pl.when(self.goes)(self.on[k].start)

    def edges(self, k):
        pl.when(self.comes)(self.on[k].wait_recv)
        mate, row = self.mate_in[k], self.row_in[k]
        entering = jnp.where(self.entry, row, mate[:BLOCK] + row * mate[BLOCK : BLOCK + 1])
        _, trail = self.sides(k)
        at_lead = trail[:BLOCK] + entering * trail[BLOCK : BLOCK + 1]
        self.back[k] = jnp.where(self.lead, entering, at_lead)
        self.three[k].start()
        self.result[self.mine[k]] = jnp.where(self.lead, at_lead, entering)

    def arrive(self, k):
        self.three[k].wait_recv()

    def finish(self):
        for k in range(4):
            self.one[k].wait_send()
            self.two[k].wait_send()
            pl.when(self.goes)(self.on[k].wait_send)
            self.three[k].wait_send()

    def serve(self, step, plan):
        for at, name, k in plan:
            pl.when(step == at)(functools.partial(getattr(self, name), k))


FORWARD_PLAN = (
    (0, "pair_totals", 0),
    (1, "pair_totals", 1),
    (2, "pair_totals", 2),
    (3, "pair_totals", 3),
    (4, "row_totals", 0),
    (5, "row_totals", 1),
    (6, "row_totals", 2),
    (8, "row_totals", 3),
    (8, "edges", 0),
    (9, "edges", 1),
    (10, "edges", 2),
    (12, "edges", 3),
)
BACKWARD_PLAN = (
    (0, "pair_totals", 0),
    (1, "pair_totals", 1),
    (2, "pair_totals", 2),
    (4, "pair_totals", 3),
    (4, "row_totals", 0),
    (5, "row_totals", 1),
    (6, "row_totals", 2),
    (7, "row_totals", 3),
    (7, "edges", 0),
    (8, "edges", 1),
    (9, "edges", 2),
    (10, "edges", 3),
)


def main_kernel(
    full_width,
    lengths_in, rates_in, gain_in, queries, keys, values, out_grad,
    normed, grad_query, key_part, value_part, key_dev, value_dev, beyond,
    lengths, rates, gain, query, key, value, cotangent, raw, scaled, weights, probs_t, query_in_t, query_dev, query_dev_t,
    key_in, grad_raw, ahead, state_local, state_half_t, chain, inverse_at, pull_at,
    running, entering_gain, leaving_gain, keeping, before, after, documents,
    own_f, first_f, totals_f, mate_f, row_f, row_in_f, back_f, entering,
    own_b, first_b, totals_b, mate_b, row_b, row_in_b, back_b,
    sums, sums_in,
    load_sem, send_f, recv_f, send_b, recv_b, send_h, recv_h,
):
    value_in = cotangent
    x, z, head = lax.axis_index("x"), lax.axis_index("z"), lax.axis_index("head")
    me = x * 4 + z
    half = HEADS // 2 * BLOCK
    mine_first = jnp.where((z == 0) | (z == 3), 0, half)
    first, second = (pl.ds(pl.multiple_of(at, half), half) for at in (half - mine_first, mine_first))
    loads = [
        pltpu.make_async_copy(source, target, load_sem.at[i])
        for i, (source, target) in enumerate(
            (
                (rates_in, rates),
                (lengths_in, lengths),
                (keys.at[:, first], key.at[:, first]),
                (values.at[:, first], value.at[:, first]),
                (keys.at[:, second], key.at[:, second]),
                (values.at[:, second], value.at[:, second]),
                (gain_in, gain),
                (queries, query),
                (out_grad, cotangent),
            )
        )
    ]
    for load in loads[:6]:
        load.start()
    barrier = pltpu.get_barrier_semaphore()
    peers = [(x, z + 1 - 2 * lax.rem(z, 2), head), (x, 3 - z, head)]
    peers += [(lax.rem(x + step, 4), z, head) for step in (1, 3)]
    peers += [(x, z, lax.rem(head + j, 8)) for j in range(1, 8)]
    for peer in peers:
        pl.semaphore_signal(barrier, inc=1, device_id=peer, device_id_type=MESH)

    loads[0].wait()
    loads[1].wait()
    lane = lax.broadcasted_iota(jnp.int32, (BLOCK, BLOCK), 1)
    sublane = lax.broadcasted_iota(jnp.int32, (BLOCK, BLOCK), 0)
    upto = (sublane <= lane).astype(F32).astype(BF16)
    rate = jnp.concatenate([rates[:, static_rows(b)] for b in range(BLOCKS)])
    top = rate.astype(BF16)
    rest = rate - top.astype(F32)
    middle = rest.astype(BF16)
    low = (rest - middle.astype(F32)).astype(BF16)
    pieces = dot(jnp.concatenate([top, middle, low]), upto)
    count = HEADS * BLOCKS
    run = pieces[:count] + pieces[count : 2 * count] + pieces[2 * count :]
    block_start = me * (BLOCKS * BLOCK) + BLOCK * lax.broadcasted_iota(jnp.int32, (BLOCKS, BLOCK), 0)
    places = block_start + lax.broadcasted_iota(jnp.int32, (BLOCKS, BLOCK), 1)
    doc = jnp.zeros((BLOCKS, BLOCK), jnp.int32)
    doc_first, doc_last = doc, doc
    end = jnp.int32(0)
    for i in range(lengths.shape[0]):
        end = end + lengths[i]
        doc += (places >= end).astype(jnp.int32)
        doc_first += (block_start - 1 >= end).astype(jnp.int32)
        doc_last += (block_start + (BLOCK - 1) >= end).astype(jnp.int32)
    doc_first = jnp.where(block_start > 0, doc_first, -1)
    documents[...] = doc.astype(F32)
    enter_mask = (doc == doc_first).astype(F32)
    leave_mask = (doc == doc_last).astype(F32)
    keep_mask = (doc_last == doc_first).astype(F32)
    so_far = jnp.ones((HEADS, BLOCK), F32)
    for b in range(BLOCKS):
        run_b = run[b * HEADS : (b + 1) * HEADS]
        total = jnp.broadcast_to(run_b[:, BLOCK - 1 :], (HEADS, BLOCK))
        running[b] = run_b
        entering_gain[b] = jnp.exp(run_b) * enter_mask[b : b + 1]
        leaving_gain[b] = jnp.exp(total - run_b) * leave_mask[b : b + 1]
        keep = jnp.exp(total) * keep_mask[b : b + 1]
        keeping[b] = keep
        before[b] = so_far
        so_far = so_far * keep
    remaining = jnp.ones((HEADS, BLOCK), F32)
    for b in reversed(range(BLOCKS)):
        after[b] = remaining
        remaining = remaining * keeping[b]
    for h in range(HEADS):
        tile = jnp.broadcast_to(so_far[h : h + 1], (8, BLOCK))
        own_f[h, BLOCK:] = tile
        own_b[h, BLOCK:] = tile

    forward = Exchange(1, own_f, first_f, totals_f, mate_f, row_f, row_in_f, back_f, entering, send_f, recv_f)
    backward = Exchange(-1, own_b, first_b, totals_b, mate_b, row_b, row_in_b, back_b, beyond, send_b, recv_b)

    forward.prepare()
    backward.prepare()

    loads[2].wait()
    loads[3].wait()
    for turn, h in enumerate(forward.other + forward.mine):
        if turn == 4:
            for load in loads[4:6]:
                load.wait()
            for load in loads[6:]:
                load.start()
        lanes = rows_of(h)
        pieces = []
        for b in range(BLOCKS):
            leave = leaving_gain[b, pl.ds(h, 1)] * after[b, pl.ds(h, 1)]
            pieces.append((jnp.transpose(key[static_rows(b), lanes]).astype(F32) * leave).astype(BF16))
        own_f[h, :BLOCK] = dot(jnp.concatenate(pieces, axis=1), value[:, lanes])
        if turn == 0:
            pl.semaphore_wait(barrier, len(peers))
        if turn < 4:
            forward.start(turn)
    chain[...] = jnp.zeros_like(chain)
    for load in loads[6:]:
        load.wait()

    last_step = 2 * BLOCKS - 1

    def local_scores(step):
        b, group = lax.div(step, 2), lax.rem(step, 2)
        rows = rows_of(b)
        doc_row = documents[pl.ds(b, 1), :]
        same = (sublane >= lane) & (as_columns(doc_row) == jnp.broadcast_to(doc_row, (BLOCK, BLOCK)))
        bias = jnp.where(same, 0.0, MASKED)
        for j in range(HEADS // 2):
            h = group * (HEADS // 2) + j
            lanes = rows_of(h)
            query_b, key_b, value_b = query[rows, lanes], key[rows, lanes], value[rows, lanes]
            run_row = running[b, pl.ds(h, 1)]
            weight = jnp.exp(as_columns(run_row) - run_row + bias)
            weights[b, h] = weight
            probs = (dot(query_b, key_b, 1, 1) * weight).astype(BF16)
            ahead[0, j] = probs
            probs_t[b, h] = jnp.transpose(probs)
            query_e = query_b.astype(F32) * as_columns(entering_gain[b, pl.ds(h, 1)])
            query_in = query_e.astype(BF16)
            ahead[1, j] = query_in
            query_in_t[b, h] = jnp.transpose(query_in)
            query_d = (query_e * before[b, pl.ds(h, 1)]).astype(BF16)
            query_dev[rows, lanes] = query_d
            query_dev_t[h, :, rows] = jnp.transpose(query_d)
            leave = as_columns(leaving_gain[b, pl.ds(h, 1)])
            after_row = after[b, pl.ds(h, 1)]
            key_l = key_b.astype(F32) * leave
            key_lb = key_l.astype(BF16)
            key_in[rows, lanes] = key_lb
            ahead[2, j] = jnp.transpose(key_lb)
            key_dev[rows, lanes] = (key_l * after_row).astype(BF16)
            scaled[rows, lanes] = cotangent[rows, lanes].astype(F32) * gain[:, lanes]
            value_l = value_b.astype(F32) * leave
            value_in[rows, lanes] = value_l.astype(BF16)
            value_dev[rows, lanes] = (value_l * after_row).astype(BF16)

    def local(step):
        b, group = lax.div(step, 2), lax.rem(step, 2)
        rows = rows_of(b)
        for j in range(HEADS // 2):
            h = group * (HEADS // 2) + j
            lanes = rows_of(h)
            value_b = value[rows, lanes]
            state = chain[h]
            state_local[b, h] = state
            raw[rows, lanes] = dot(
                jnp.concatenate([ahead[0, j], ahead[1, j]], axis=1), jnp.concatenate([value_b, state.astype(BF16)])
            )
            chain[h] = keeping[b, pl.ds(h, 1)] * state + dot(ahead[2, j], value_b)

    def local_step(step, carry):
        local(step)
        local_scores(step + 1)
        forward.serve(step, FORWARD_PLAN)
        return carry

    local_scores(jnp.int32(0))
    lax.fori_loop(0, last_step, local_step, 0)
    local(jnp.int32(last_step))
    squares, projected = inverse_at, pull_at
    squares[...] = jnp.zeros_like(squares)
    projected[...] = jnp.zeros_like(projected)

    def finish_raw(h):
        lanes = rows_of(h)
        added = dot(query_dev[:, lanes], entering[h].astype(BF16))
        for b in range(BLOCKS):
            rows = static_rows(b)
            out = raw[rows, lanes] + added[rows]
            raw[rows, lanes] = out
            squares[b] += out * out
            projected[b] += out * scaled[rows, lanes]

    for k in range(4):
        finish_raw(forward.mine[k])
    for k in range(4):
        forward.arrive(k)
        finish_raw(forward.other[k])
    for b in range(BLOCKS):
        sums[0, b : b + 1] = jnp.sum(jnp.transpose(squares[b]), axis=0, keepdims=True)
        sums[1, b : b + 1] = jnp.sum(jnp.transpose(projected[b]), axis=0, keepdims=True)
    shares = []
    for j in range(1, 8):
        shares.append(
            pltpu.make_async_remote_copy(
                src_ref=sums,
                dst_ref=sums_in.at[j - 1],
                send_sem=send_h.at[j - 1],
                recv_sem=recv_h.at[j - 1],
                device_id=(x, z, lax.rem(head + j, 8)),
                device_id_type=MESH,
            )
        )
        shares[-1].start()
    forward.finish()
    chain[...] = jnp.zeros_like(chain)

    def whole_states(b, carry):
        for h in range(HEADS):
            state = state_local[b, h] + before[b, h : h + 1] * entering[h]
            state_half_t[b, h] = jnp.transpose(state.astype(BF16))
        return carry

    lax.fori_loop(0, BLOCKS, whole_states, 0)
    total = sums[...]
    for j in range(7):
        shares[j].wait_recv()
        total = total + sums_in[j]
    inverse = lax.rsqrt(total[0] / full_width + epsilon)
    pull = inverse * inverse * inverse * total[1] / full_width
    for b in range(BLOCKS):
        inverse_at[b] = as_columns(inverse[b : b + 1])
        pull_at[b] = as_columns(pull[b : b + 1])
    for turn, h in enumerate(backward.other + backward.mine):
        lanes = rows_of(h)
        pieces = []
        for b in range(BLOCKS):
            rows = static_rows(b)
            grad = (inverse_at[b] * scaled[rows, lanes] - raw[rows, lanes] * pull_at[b]).astype(BF16)
            grad_raw[rows, lanes] = grad
            pieces.append(grad)
        own_b[h, :BLOCK] = dot(query_dev_t[h], jnp.concatenate(pieces))
        if turn < 4:
            backward.start(turn)
    for j in range(7):
        shares[j].wait_send()

    def gradient_scores(step):
        b, group = BLOCKS - 1 - lax.div(step, 2), lax.rem(step, 2)
        rows = rows_of(b)
        for j in range(HEADS // 2):
            h = group * (HEADS // 2) + j
            lanes = rows_of(h)
            grad = grad_raw[rows, lanes]
            mixed = (dot(grad, value[rows, lanes], 1, 1) * weights[b, h]).astype(BF16)
            ahead[0, j] = mixed
            ahead[1, j] = jnp.transpose(mixed)
            ahead[2, j] = (grad.astype(F32) * as_columns(entering_gain[b, pl.ds(h, 1)])).astype(BF16)

    def gradients(step):
        b, group = BLOCKS - 1 - lax.div(step, 2), lax.rem(step, 2)
        rows = rows_of(b)
        for j in range(HEADS // 2):
            h = group * (HEADS // 2) + j
            lanes = rows_of(h)
            grad = grad_raw[rows, lanes]
            grad_query[rows, lanes] = dot(
                jnp.concatenate([ahead[0, j], ahead[2, j]], axis=1),
                jnp.concatenate([key[rows, lanes], state_half_t[b, h]]),
            ).astype(BF16)
            carried = chain[h]
            carried_half = carried.astype(BF16)
            key_part[rows, lanes] = dot(
                jnp.concatenate([ahead[1, j], value_in[rows, lanes]], axis=1),
                jnp.concatenate([query[rows, lanes], jnp.transpose(carried_half)]),
            )
            value_part[rows, lanes] = dot(
                jnp.concatenate([probs_t[b, h], key_in[rows, lanes]], axis=1),
                jnp.concatenate([grad, carried_half]),
            )
            chain[h] = keeping[b, pl.ds(h, 1)] * carried + dot(query_in_t[b, h], grad)
            normed[rows, lanes] = (raw[rows, lanes] * inverse_at[b] * gain[:, lanes]).astype(BF16)

    def gradient_step(step, carry):
        gradients(step)
        gradient_scores(step + 1)
        backward.serve(step, BACKWARD_PLAN)
        return carry

    gradient_scores(jnp.int32(0))
    lax.fori_loop(0, last_step, gradient_step, 0)
    gradients(jnp.int32(last_step))
    for k in range(4):
        backward.arrive(k)
    backward.finish()


def last_kernel(
    normed_in, query_in, key_part, value_part, key_dev, value_dev, beyond,
    normed, grad_query, grad_key, grad_value,
    key_rows, value_rows, plain, turned, pass_sem, key_sem, value_sem,
):
    passes = [
        pltpu.make_async_copy(normed_in, normed, pass_sem.at[0]),
        pltpu.make_async_copy(query_in, grad_query, pass_sem.at[1]),
    ]
    for copy in passes:
        copy.start()

    tall = 2 * BLOCK

    def stores(b):
        rows = pl.ds(pl.multiple_of(b * tall, tall), tall)
        return (
            pltpu.make_async_copy(key_rows.at[rows], grad_key.at[rows], key_sem.at[b]),
            pltpu.make_async_copy(value_rows.at[rows], grad_value.at[rows], value_sem.at[b]),
        )

    zero = jnp.zeros((BLOCK, BLOCK), BF16)
    for h in range(HEADS):
        state = beyond[h].astype(BF16)
        for states, part in ((plain, state), (turned, jnp.transpose(state))):
            pair = (part, zero) if h % 2 == 0 else (zero, part)
            states[h // 2, static_rows(h % 2)] = jnp.concatenate(pair, axis=1)

    def block(b, carry):
        rows = pl.ds(pl.multiple_of(b * tall, tall), tall)
        for pair in range(HEADS // 2):
            lanes = slice(pair * tall, (pair + 1) * tall)
            key_rows[rows, lanes] = (key_part[rows, lanes] + dot(value_dev[rows, lanes], turned[pair])).astype(BF16)
            value_rows[rows, lanes] = (value_part[rows, lanes] + dot(key_dev[rows, lanes], plain[pair])).astype(BF16)
        for copy in stores(b):
            copy.start()
        return carry

    lax.fori_loop(0, BLOCKS // 2, block, 0)
    for copy in passes:
        copy.wait()

    def settle(b, carry):
        for copy in stores(b):
            copy.wait()
        return carry

    lax.fori_loop(0, BLOCKS // 2, settle, 0)


def body(queries, keys, values, log_decay, gain, lengths, out_grad):
    rows, width = queries.shape
    full_width = width * lax.axis_size("head")
    vmem = pl.BlockSpec(memory_space=pltpu.VMEM)
    hbm = pl.BlockSpec(memory_space=pl.ANY)
    wide = (rows, width)
    tiles = (BLOCKS, HEADS, BLOCK, BLOCK)
    small = pltpu.VMEM((BLOCKS, HEADS, BLOCK), F32)
    own = pltpu.VMEM((HEADS, SLAB, BLOCK), F32)
    slab = pltpu.VMEM((4, SLAB, BLOCK), F32)
    states = pltpu.VMEM((HEADS, BLOCK, BLOCK), F32)
    part = pltpu.VMEM((4, BLOCK, BLOCK), F32)
    wires = [own, slab, slab, slab, part, part, part]
    half, full = pltpu.VMEM(wide, BF16), pltpu.VMEM(wide, F32)
    handed = (half, half, full, full, half, half, states)
    two_heads = pltpu.VMEM((HEADS // 2, 2 * BLOCK, 2 * BLOCK), BF16)
    dma = pltpu.SemaphoreType.DMA
    found = pl.pallas_call(
        functools.partial(main_kernel, full_width),
        out_shape=handed,
        in_specs=[hbm] * 7,
        out_specs=(vmem,) * len(handed),
        scratch_shapes=[
            pltpu.SMEM((8,), jnp.int32),
            pltpu.VMEM((HEADS, rows), F32),
            pltpu.VMEM((1, width), F32),
            half, half, half, half, full, full,
            pltpu.VMEM(tiles, F32),
            pltpu.VMEM(tiles, BF16),
            pltpu.VMEM(tiles, BF16),
            half,
            pltpu.VMEM((HEADS, BLOCK, rows), BF16),
            half, half,
            pltpu.VMEM((3, HEADS // 2, BLOCK, BLOCK), BF16),
            pltpu.VMEM(tiles, F32),
            pltpu.VMEM(tiles, BF16),
            states, states, states,
            small, small, small, small, small, small,
            pltpu.VMEM((BLOCKS, BLOCK), F32),
            *wires,
            states,
            *wires,
            pltpu.VMEM((2, BLOCKS, BLOCK), F32),
            pltpu.VMEM((7, 2, BLOCKS, BLOCK), F32),
            dma((9,)),
            dma((16,)),
            dma((16,)),
            dma((16,)),
            dma((16,)),
            dma((7,)),
            dma((7,)),
        ],
        compiler_params=pltpu.CompilerParams(
            collective_id=0, has_side_effects=True, vmem_limit_bytes=46 * 2**20
        ),
        name="main_kernel",
    )(lengths, log_decay.T, gain.reshape(1, width), queries, keys, values, out_grad)
    return pl.pallas_call(
        last_kernel,
        out_shape=(jax.ShapeDtypeStruct(wide, BF16),) * 4,
        in_specs=[vmem] * len(handed),
        out_specs=(hbm,) * 4,
        scratch_shapes=[half, half, two_heads, two_heads, dma((2,)), dma((4,)), dma((4,))],
        compiler_params=pltpu.CompilerParams(vmem_limit_bytes=8 * 2**20),
        name="last_kernel",
    )(*found)


def solution(mesh):
    split = Mesh(mesh.devices.reshape(4, 4, mesh.shape["head"]), ("x", "z", "head"))
    wide = P(SEQ, "head")
    return jax.shard_map(
        body,
        mesh=split,
        in_specs=(wide, wide, wide, wide, P("head"), P(), wide),
        out_specs=(wide,) * 4,
        check_vma=False,
    )
```

```python
import functools

import jax
import jax.numpy as jnp
from jax import lax
from jax.experimental import pallas as pl
from jax.experimental.pallas import tpu as pltpu
from jax.sharding import Mesh
from jax.sharding import PartitionSpec as P

BLOCK = 128
HEADS = 8
BLOCKS = 8
SEQ = ("x", "z")
MESH = pl.DeviceIdType.MESH
F32 = jnp.float32
BF16 = jnp.bfloat16
epsilon = 1e-06
MASKED = -1e30
SLAB = BLOCK + 8


def dot(left, right, left_axis=1, right_axis=0):
    dims = (((left_axis,), (right_axis,)), ((), ()))
    return lax.dot_general(left, right, dims, preferred_element_type=F32)


def rows_of(block):
    return pl.ds(pl.multiple_of(block * BLOCK, BLOCK), BLOCK)


def static_rows(block):
    return slice(block * BLOCK, (block + 1) * BLOCK)


def as_columns(row):
    return jnp.transpose(jnp.broadcast_to(row, (BLOCK, BLOCK)))


class Exchange:
    def __init__(self, step, own, first_in, totals, mate_in, row, row_in, back, result, send, recv):
        self.own, self.first_in, self.totals, self.mate_in = own, first_in, totals, mate_in
        self.row, self.row_in, self.back, self.result = row, row_in, back, result
        x, z, head = lax.axis_index("x"), lax.axis_index("z"), lax.axis_index("head")
        odd = lax.rem(z, 2)
        half = jnp.where((z == 0) | (z == 3), 0, 1)
        self.mine = [4 * half + k for k in range(4)]
        self.other = [4 * (1 - half) + k for k in range(4)]
        self.lead = odd == (1 if step == 1 else 0)
        self.entry = z < 2 if step == 1 else z >= 2
        self.goes = x < 3 if step == 1 else x > 0
        self.comes = x > 0 if step == 1 else x < 3
        partner = (x, z + 1 - 2 * odd, head)
        mate = (x, 3 - z, head)
        onward = (lax.rem(x + step + 4, 4), z, head)

        def copy(source, target, index, device):
            return pltpu.make_async_remote_copy(
                src_ref=source,
                dst_ref=target,
                send_sem=send.at[index],
                recv_sem=recv.at[index],
                device_id=device,
                device_id_type=MESH,
            )

        self.one, self.two, self.on, self.three = [], [], [], []
        for k in range(4):
            self.one.append(copy(own.at[self.other[k]], first_in.at[k], k, partner))
            self.two.append(copy(totals.at[k], mate_in.at[k], 4 + k, mate))
            self.on.append(copy(row.at[k], row_in.at[k], 8 + k, onward))
            self.three.append(copy(back.at[k], result.at[self.mine[k]], 12 + k, partner))

    def prepare(self):
        @pl.when(jnp.logical_not(self.comes))
        def _():
            self.row_in[...] = jnp.zeros_like(self.row_in)

    def start(self, k):
        self.one[k].start()

    def sides(self, k):
        mine, theirs = self.own[self.mine[k]], self.first_in[k]
        return jnp.where(self.lead, mine, theirs), jnp.where(self.lead, theirs, mine)

    def pair_totals(self, k):
        self.one[k].wait_recv()
        lead, trail = self.sides(k)
        total = lead[:BLOCK] + trail[:BLOCK] * lead[BLOCK : BLOCK + 1]
        self.totals[k, :BLOCK] = total
        self.totals[k, BLOCK:] = lead[BLOCK:] * trail[BLOCK:]
        self.two[k].start()

        @pl.when(jnp.logical_not(self.entry))
        def _():
            self.row[k] = total
            pl.when(self.goes)(self.on[k].start)

    def row_totals(self, k):
        self.two[k].wait_recv()

        @pl.when(self.entry)
        def _():
            mate = self.mate_in[k]
            self.row[k] = mate[:BLOCK] + self.totals[k, :BLOCK] * mate[BLOCK : BLOCK + 1]
            pl.when(self.goes)(self.on[k].start)

    def edges(self, k):
        pl.when(self.comes)(self.on[k].wait_recv)
        mate, row = self.mate_in[k], self.row_in[k]
        entering = jnp.where(self.entry, row, mate[:BLOCK] + row * mate[BLOCK : BLOCK + 1])
        _, trail = self.sides(k)
        at_lead = trail[:BLOCK] + entering * trail[BLOCK : BLOCK + 1]
        self.back[k] = jnp.where(self.lead, entering, at_lead)
        self.three[k].start()
        self.result[self.mine[k]] = jnp.where(self.lead, at_lead, entering)

    def arrive(self, k):
        self.three[k].wait_recv()

    def finish(self):
        for k in range(4):
            self.one[k].wait_send()
            self.two[k].wait_send()
            pl.when(self.goes)(self.on[k].wait_send)
            self.three[k].wait_send()

    def serve(self, step, plan):
        for at, name, k in plan:
            pl.when(step == at)(functools.partial(getattr(self, name), k))


FORWARD_PLAN = (
    (0, "pair_totals", 0),
    (1, "pair_totals", 1),
    (2, "pair_totals", 2),
    (3, "pair_totals", 3),
    (4, "row_totals", 0),
    (5, "row_totals", 1),
    (6, "row_totals", 2),
    (8, "row_totals", 3),
    (8, "edges", 0),
    (9, "edges", 1),
    (10, "edges", 2),
    (12, "edges", 3),
)
BACKWARD_PLAN = (
    (0, "pair_totals", 0),
    (1, "pair_totals", 1),
    (2, "pair_totals", 2),
    (4, "pair_totals", 3),
    (4, "row_totals", 0),
    (5, "row_totals", 1),
    (6, "row_totals", 2),
    (7, "row_totals", 3),
    (7, "edges", 0),
    (8, "edges", 1),
    (9, "edges", 2),
    (10, "edges", 3),
)


def main_kernel(
    full_width,
    lengths_in, rates_in, gain_in, queries, keys, values, out_grad,
    normed, grad_query, key_part, value_part, key_dev, value_dev, beyond,
    lengths, rates, gain, query, key, value, cotangent, raw, scaled, weights, probs_t, query_in_t, query_dev, query_dev_t,
    key_in, grad_raw, ahead, state_local, state_half_t, chain, inverse_at, pull_at,
    running, entering_gain, leaving_gain, keeping, before, after, documents,
    own_f, first_f, totals_f, mate_f, row_f, row_in_f, back_f, entering,
    own_b, first_b, totals_b, mate_b, row_b, row_in_b, back_b,
    sums, sums_in,
    load_sem, send_f, recv_f, send_b, recv_b, send_h, recv_h,
):
    value_in = cotangent
    x, z, head = lax.axis_index("x"), lax.axis_index("z"), lax.axis_index("head")
    me = x * 4 + z
    half = HEADS // 2 * BLOCK
    mine_first = jnp.where((z == 0) | (z == 3), 0, half)
    first, second = (pl.ds(pl.multiple_of(at, half), half) for at in (half - mine_first, mine_first))
    loads = [
        pltpu.make_async_copy(source, target, load_sem.at[i])
        for i, (source, target) in enumerate(
            (
                (rates_in, rates),
                (lengths_in, lengths),
                (keys.at[:, first], key.at[:, first]),
                (values.at[:, first], value.at[:, first]),
                (keys.at[:, second], key.at[:, second]),
                (values.at[:, second], value.at[:, second]),
                (gain_in, gain),
                (queries, query),
                (out_grad, cotangent),
            )
        )
    ]
    for load in loads[:6]:
        load.start()
    barrier = pltpu.get_barrier_semaphore()
    peers = [(x, z + 1 - 2 * lax.rem(z, 2), head), (x, 3 - z, head)]
    peers += [(lax.rem(x + step, 4), z, head) for step in (1, 3)]
    peers += [(x, z, lax.rem(head + j, 8)) for j in range(1, 8)]
    for peer in peers:
        pl.semaphore_signal(barrier, inc=1, device_id=peer, device_id_type=MESH)

    loads[0].wait()
    loads[1].wait()
    lane = lax.broadcasted_iota(jnp.int32, (BLOCK, BLOCK), 1)
    sublane = lax.broadcasted_iota(jnp.int32, (BLOCK, BLOCK), 0)
    upto = (sublane <= lane).astype(F32).astype(BF16)
    rate = jnp.concatenate([rates[:, static_rows(b)] for b in range(BLOCKS)])
    top = rate.astype(BF16)
    rest = rate - top.astype(F32)
    middle = rest.astype(BF16)
    low = (rest - middle.astype(F32)).astype(BF16)
    pieces = dot(jnp.concatenate([top, middle, low]), upto)
    count = HEADS * BLOCKS
    run = pieces[:count] + pieces[count : 2 * count] + pieces[2 * count :]
    block_start = me * (BLOCKS * BLOCK) + BLOCK * lax.broadcasted_iota(jnp.int32, (BLOCKS, BLOCK), 0)
    places = block_start + lax.broadcasted_iota(jnp.int32, (BLOCKS, BLOCK), 1)
    doc = jnp.zeros((BLOCKS, BLOCK), jnp.int32)
    doc_first, doc_last = doc, doc
    end = jnp.int32(0)
    for i in range(lengths.shape[0]):
        end = end + lengths[i]
        doc += (places >= end).astype(jnp.int32)
        doc_first += (block_start - 1 >= end).astype(jnp.int32)
        doc_last += (block_start + (BLOCK - 1) >= end).astype(jnp.int32)
    doc_first = jnp.where(block_start > 0, doc_first, -1)
    documents[...] = doc.astype(F32)
    enter_mask = (doc == doc_first).astype(F32)
    leave_mask = (doc == doc_last).astype(F32)
    keep_mask = (doc_last == doc_first).astype(F32)
    so_far = jnp.ones((HEADS, BLOCK), F32)
    for b in range(BLOCKS):
        run_b = run[b * HEADS : (b + 1) * HEADS]
        total = jnp.broadcast_to(run_b[:, BLOCK - 1 :], (HEADS, BLOCK))
        running[b] = run_b
        entering_gain[b] = jnp.exp(run_b) * enter_mask[b : b + 1]
        leaving_gain[b] = jnp.exp(total - run_b) * leave_mask[b : b + 1]
        keep = jnp.exp(total) * keep_mask[b : b + 1]
        keeping[b] = keep
        before[b] = so_far
        so_far = so_far * keep
    remaining = jnp.ones((HEADS, BLOCK), F32)
    for b in reversed(range(BLOCKS)):
        after[b] = remaining
        remaining = remaining * keeping[b]
    for h in range(HEADS):
        tile = jnp.broadcast_to(so_far[h : h + 1], (8, BLOCK))
        own_f[h, BLOCK:] = tile
        own_b[h, BLOCK:] = tile

    forward = Exchange(1, own_f, first_f, totals_f, mate_f, row_f, row_in_f, back_f, entering, send_f, recv_f)
    backward = Exchange(-1, own_b, first_b, totals_b, mate_b, row_b, row_in_b, back_b, beyond, send_b, recv_b)

    forward.prepare()
    backward.prepare()

    loads[2].wait()
    loads[3].wait()
    for load in loads[6:]:
        load.start()
    for turn, h in enumerate(forward.other + forward.mine):
        if turn == 4:
            for load in loads[4:6]:
                load.wait()
        lanes = rows_of(h)
        pieces = []
        for b in range(BLOCKS):
            leave = leaving_gain[b, pl.ds(h, 1)] * after[b, pl.ds(h, 1)]
            pieces.append((jnp.transpose(key[static_rows(b), lanes]).astype(F32) * leave).astype(BF16))
        own_f[h, :BLOCK] = dot(jnp.concatenate(pieces, axis=1), value[:, lanes])
        if turn == 0:
            pl.semaphore_wait(barrier, len(peers))
        if turn < 4:
            forward.start(turn)
    chain[...] = jnp.zeros_like(chain)
    for load in loads[6:]:
        load.wait()

    last_step = 2 * BLOCKS - 1

    def local_scores(step):
        b, group = lax.div(step, 2), lax.rem(step, 2)
        rows = rows_of(b)
        doc_row = documents[pl.ds(b, 1), :]
        same = (sublane >= lane) & (as_columns(doc_row) == jnp.broadcast_to(doc_row, (BLOCK, BLOCK)))
        bias = jnp.where(same, 0.0, MASKED)
        for j in range(HEADS // 2):
            h = group * (HEADS // 2) + j
            lanes = rows_of(h)
            query_b, key_b, value_b = query[rows, lanes], key[rows, lanes], value[rows, lanes]
            run_row = running[b, pl.ds(h, 1)]
            weight = jnp.exp(as_columns(run_row) - run_row + bias)
            weights[b, h] = weight
            probs = (dot(query_b, key_b, 1, 1) * weight).astype(BF16)
            ahead[0, j] = probs
            probs_t[b, h] = jnp.transpose(probs)
            query_e = query_b.astype(F32) * as_columns(entering_gain[b, pl.ds(h, 1)])
            query_in = query_e.astype(BF16)
            ahead[1, j] = query_in
            query_in_t[b, h] = jnp.transpose(query_in)
            query_d = (query_e * before[b, pl.ds(h, 1)]).astype(BF16)
            query_dev[rows, lanes] = query_d
            query_dev_t[h, :, rows] = jnp.transpose(query_d)
            leave = as_columns(leaving_gain[b, pl.ds(h, 1)])
            after_row = after[b, pl.ds(h, 1)]
            key_l = key_b.astype(F32) * leave
            key_lb = key_l.astype(BF16)
            key_in[rows, lanes] = key_lb
            ahead[2, j] = jnp.transpose(key_lb)
            key_dev[rows, lanes] = (key_l * after_row).astype(BF16)
            scaled[rows, lanes] = cotangent[rows, lanes].astype(F32) * gain[:, lanes]
            value_l = value_b.astype(F32) * leave
            value_in[rows, lanes] = value_l.astype(BF16)
            value_dev[rows, lanes] = (value_l * after_row).astype(BF16)

    def local(step):
        b, group = lax.div(step, 2), lax.rem(step, 2)
        rows = rows_of(b)
        for j in range(HEADS // 2):
            h = group * (HEADS // 2) + j
            lanes = rows_of(h)
            value_b = value[rows, lanes]
            state = chain[h]
            state_local[b, h] = state
            raw[rows, lanes] = dot(
                jnp.concatenate([ahead[0, j], ahead[1, j]], axis=1), jnp.concatenate([value_b, state.astype(BF16)])
            )
            chain[h] = keeping[b, pl.ds(h, 1)] * state + dot(ahead[2, j], value_b)

    def local_step(step, carry):
        local(step)
        local_scores(step + 1)
        forward.serve(step, FORWARD_PLAN)
        return carry

    local_scores(jnp.int32(0))
    lax.fori_loop(0, last_step, local_step, 0)
    local(jnp.int32(last_step))
    squares, projected = inverse_at, pull_at
    squares[...] = jnp.zeros_like(squares)
    projected[...] = jnp.zeros_like(projected)

    def finish_raw(h):
        lanes = rows_of(h)
        added = dot(query_dev[:, lanes], entering[h].astype(BF16))
        for b in range(BLOCKS):
            rows = static_rows(b)
            out = raw[rows, lanes] + added[rows]
            raw[rows, lanes] = out
            squares[b] += out * out
            projected[b] += out * scaled[rows, lanes]

    for k in range(4):
        finish_raw(forward.mine[k])
    for k in range(4):
        forward.arrive(k)
        finish_raw(forward.other[k])
    for b in range(BLOCKS):
        sums[0, b : b + 1] = jnp.sum(jnp.transpose(squares[b]), axis=0, keepdims=True)
        sums[1, b : b + 1] = jnp.sum(jnp.transpose(projected[b]), axis=0, keepdims=True)
    shares = []
    for j in range(1, 8):
        shares.append(
            pltpu.make_async_remote_copy(
                src_ref=sums,
                dst_ref=sums_in.at[j - 1],
                send_sem=send_h.at[j - 1],
                recv_sem=recv_h.at[j - 1],
                device_id=(x, z, lax.rem(head + j, 8)),
                device_id_type=MESH,
            )
        )
        shares[-1].start()
    forward.finish()
    chain[...] = jnp.zeros_like(chain)

    def whole_states(b, carry):
        for h in range(HEADS):
            state = state_local[b, h] + before[b, h : h + 1] * entering[h]
            state_half_t[b, h] = jnp.transpose(state.astype(BF16))
        return carry

    lax.fori_loop(0, BLOCKS, whole_states, 0)
    total = sums[...]
    for j in range(7):
        shares[j].wait_recv()
        total = total + sums_in[j]
    inverse = lax.rsqrt(total[0] / full_width + epsilon)
    pull = inverse * inverse * inverse * total[1] / full_width
    for b in range(BLOCKS):
        inverse_at[b] = as_columns(inverse[b : b + 1])
        pull_at[b] = as_columns(pull[b : b + 1])
    for turn, h in enumerate(backward.other + backward.mine):
        lanes = rows_of(h)
        pieces = []
        for b in range(BLOCKS):
            rows = static_rows(b)
            grad = (inverse_at[b] * scaled[rows, lanes] - raw[rows, lanes] * pull_at[b]).astype(BF16)
            grad_raw[rows, lanes] = grad
            pieces.append(grad)
        own_b[h, :BLOCK] = dot(query_dev_t[h], jnp.concatenate(pieces))
        if turn < 4:
            backward.start(turn)
    for j in range(7):
        shares[j].wait_send()

    def gradient_scores(step):
        b, group = BLOCKS - 1 - lax.div(step, 2), lax.rem(step, 2)
        rows = rows_of(b)
        for j in range(HEADS // 2):
            h = group * (HEADS // 2) + j
            lanes = rows_of(h)
            grad = grad_raw[rows, lanes]
            mixed = (dot(grad, value[rows, lanes], 1, 1) * weights[b, h]).astype(BF16)
            ahead[0, j] = mixed
            ahead[1, j] = jnp.transpose(mixed)
            ahead[2, j] = (grad.astype(F32) * as_columns(entering_gain[b, pl.ds(h, 1)])).astype(BF16)

    def gradients(step):
        b, group = BLOCKS - 1 - lax.div(step, 2), lax.rem(step, 2)
        rows = rows_of(b)
        for j in range(HEADS // 2):
            h = group * (HEADS // 2) + j
            lanes = rows_of(h)
            grad = grad_raw[rows, lanes]
            grad_query[rows, lanes] = dot(
                jnp.concatenate([ahead[0, j], ahead[2, j]], axis=1),
                jnp.concatenate([key[rows, lanes], state_half_t[b, h]]),
            ).astype(BF16)
            carried = chain[h]
            carried_half = carried.astype(BF16)
            key_part[rows, lanes] = dot(
                jnp.concatenate([ahead[1, j], value_in[rows, lanes]], axis=1),
                jnp.concatenate([query[rows, lanes], jnp.transpose(carried_half)]),
            )
            value_part[rows, lanes] = dot(
                jnp.concatenate([probs_t[b, h], key_in[rows, lanes]], axis=1),
                jnp.concatenate([grad, carried_half]),
            )
            chain[h] = keeping[b, pl.ds(h, 1)] * carried + dot(query_in_t[b, h], grad)
            normed[rows, lanes] = (raw[rows, lanes] * inverse_at[b] * gain[:, lanes]).astype(BF16)

    def gradient_step(step, carry):
        gradients(step)
        gradient_scores(step + 1)
        backward.serve(step, BACKWARD_PLAN)
        return carry

    gradient_scores(jnp.int32(0))
    lax.fori_loop(0, last_step, gradient_step, 0)
    gradients(jnp.int32(last_step))
    for k in range(4):
        backward.arrive(k)
    backward.finish()


def last_kernel(
    normed_in, query_in, key_part, value_part, key_dev, value_dev, beyond,
    normed, grad_query, grad_key, grad_value,
    key_rows, value_rows, plain, turned, pass_sem, key_sem, value_sem,
):
    passes = [
        pltpu.make_async_copy(normed_in, normed, pass_sem.at[0]),
        pltpu.make_async_copy(query_in, grad_query, pass_sem.at[1]),
    ]
    for copy in passes:
        copy.start()

    tall = 2 * BLOCK

    def stores(b):
        rows = pl.ds(pl.multiple_of(b * tall, tall), tall)
        return (
            pltpu.make_async_copy(key_rows.at[rows], grad_key.at[rows], key_sem.at[b]),
            pltpu.make_async_copy(value_rows.at[rows], grad_value.at[rows], value_sem.at[b]),
        )

    zero = jnp.zeros((BLOCK, BLOCK), BF16)
    for h in range(HEADS):
        state = beyond[h].astype(BF16)
        for states, part in ((plain, state), (turned, jnp.transpose(state))):
            pair = (part, zero) if h % 2 == 0 else (zero, part)
            states[h // 2, static_rows(h % 2)] = jnp.concatenate(pair, axis=1)

    def block(b, carry):
        rows = pl.ds(pl.multiple_of(b * tall, tall), tall)
        for pair in range(HEADS // 2):
            lanes = slice(pair * tall, (pair + 1) * tall)
            key_rows[rows, lanes] = (key_part[rows, lanes] + dot(value_dev[rows, lanes], turned[pair])).astype(BF16)
            value_rows[rows, lanes] = (value_part[rows, lanes] + dot(key_dev[rows, lanes], plain[pair])).astype(BF16)
        for copy in stores(b):
            copy.start()
        return carry

    lax.fori_loop(0, BLOCKS // 2, block, 0)
    for copy in passes:
        copy.wait()

    def settle(b, carry):
        for copy in stores(b):
            copy.wait()
        return carry

    lax.fori_loop(0, BLOCKS // 2, settle, 0)


def body(queries, keys, values, log_decay, gain, lengths, out_grad):
    rows, width = queries.shape
    full_width = width * lax.axis_size("head")
    vmem = pl.BlockSpec(memory_space=pltpu.VMEM)
    hbm = pl.BlockSpec(memory_space=pl.ANY)
    wide = (rows, width)
    tiles = (BLOCKS, HEADS, BLOCK, BLOCK)
    small = pltpu.VMEM((BLOCKS, HEADS, BLOCK), F32)
    own = pltpu.VMEM((HEADS, SLAB, BLOCK), F32)
    slab = pltpu.VMEM((4, SLAB, BLOCK), F32)
    states = pltpu.VMEM((HEADS, BLOCK, BLOCK), F32)
    part = pltpu.VMEM((4, BLOCK, BLOCK), F32)
    wires = [own, slab, slab, slab, part, part, part]
    half, full = pltpu.VMEM(wide, BF16), pltpu.VMEM(wide, F32)
    handed = (half, half, full, full, half, half, states)
    two_heads = pltpu.VMEM((HEADS // 2, 2 * BLOCK, 2 * BLOCK), BF16)
    dma = pltpu.SemaphoreType.DMA
    found = pl.pallas_call(
        functools.partial(main_kernel, full_width),
        out_shape=handed,
        in_specs=[hbm] * 7,
        out_specs=(vmem,) * len(handed),
        scratch_shapes=[
            pltpu.SMEM((8,), jnp.int32),
            pltpu.VMEM((HEADS, rows), F32),
            pltpu.VMEM((1, width), F32),
            half, half, half, half, full, full,
            pltpu.VMEM(tiles, F32),
            pltpu.VMEM(tiles, BF16),
            pltpu.VMEM(tiles, BF16),
            half,
            pltpu.VMEM((HEADS, BLOCK, rows), BF16),
            half, half,
            pltpu.VMEM((3, HEADS // 2, BLOCK, BLOCK), BF16),
            pltpu.VMEM(tiles, F32),
            pltpu.VMEM(tiles, BF16),
            states, states, states,
            small, small, small, small, small, small,
            pltpu.VMEM((BLOCKS, BLOCK), F32),
            *wires,
            states,
            *wires,
            pltpu.VMEM((2, BLOCKS, BLOCK), F32),
            pltpu.VMEM((7, 2, BLOCKS, BLOCK), F32),
            dma((9,)),
            dma((16,)),
            dma((16,)),
            dma((16,)),
            dma((16,)),
            dma((7,)),
            dma((7,)),
        ],
        compiler_params=pltpu.CompilerParams(
            collective_id=0, has_side_effects=True, vmem_limit_bytes=46 * 2**20
        ),
        name="main_kernel",
    )(lengths, log_decay.T, gain.reshape(1, width), queries, keys, values, out_grad)
    return pl.pallas_call(
        last_kernel,
        out_shape=(jax.ShapeDtypeStruct(wide, BF16),) * 4,
        in_specs=[vmem] * len(handed),
        out_specs=(hbm,) * 4,
        scratch_shapes=[half, half, two_heads, two_heads, dma((2,)), dma((4,)), dma((4,))],
        compiler_params=pltpu.CompilerParams(vmem_limit_bytes=8 * 2**20),
        name="last_kernel",
    )(*found)


def solution(mesh):
    split = Mesh(mesh.devices.reshape(4, 4, mesh.shape["head"]), ("x", "z", "head"))
    wide = P(SEQ, "head")
    return jax.shard_map(
        body,
        mesh=split,
        in_specs=(wide, wide, wide, wide, P("head"), P(), wide),
        out_specs=(wide,) * 4,
        check_vma=False,
    )
```
